256 devices in a mesh: section: 8 (over y, x_lo), dp: 32 (over x_hi, z, core).
Axes of the slice: x: 4 (x_hi: 2, x_lo: 2; x = x_hi * 2 + x_lo), y: 4, z: 8, core: 2. Of those that a mesh axis runs over, the one named last changes fastest.
Arguments:
- inputs: bfloat16 [8, 2, 2048, 4096], P('section', None, 'dp'), may hold values from -6 to 6
- cotangent: bfloat16 [2, 2048, 4096], P(None, 'dp'), may hold values from -6 to 6
- norm_gain: bfloat16 [8, 4096], P('section', 'dp'), may hold values from 0.5 to 1.5
- key_weight: bfloat16 [8, 4096, 512], P('section', 'dp'), may hold values from -0.09375 to 0.09375
- value_weight: bfloat16 [8, 4096, 512], P('section', 'dp'), may hold values from -0.09375 to 0.09375
- plan: int32 [8, 2], P('section'), may hold values from 0 to 1, each once within a row
Outputs:
- grad_inputs: bfloat16 [8, 2, 2048, 4096], P('section', None, 'dp')
- key_weight_grad: float32 [8, 4096, 512], P('section', 'dp')
- value_weight_grad: float32 [8, 4096, 512], P('section', 'dp')
- gain_grad: float32 [8, 4096], P('section', 'dp')
The draws below stay inside these ranges and needn't reach their ends.
Inputs may be any that keep to these rules, and one draw needn't show every extreme that they name: Each row of plan lists every micro-batch once.
All inputs are finite; a program needn't handle non-finite values.
Results may differ from the reference program's by a relative error of at most 0.03.
Values may be sent and summed in bfloat16 or wider, within the bound.
A program may use at most 128 MiB of HBM per device.

```python
import math
import jax
import jax.numpy as jnp
from jax import lax

D = 4096
HEADS = 32
KV_HEADS = 4
HEAD_DIM = 128
KV = 512
GROUP = 8
MB = 2
TOK_DEV = 64
TOKENS = 2048
N_SECTION = 8
N_DP = 32


def strengthened(drawn, stream_key, source, target, blocks, factor):
    def block_of(position):
        return (jnp.arange(drawn.shape[position]) // (drawn.shape[position] // blocks)).reshape((-1,) + (1,) * (drawn.ndim - 1 - position))

    near = jax.random.permutation(stream_key, blocks)[block_of(target)]
    second = (block_of(target) + blocks // 2) % blocks
    return jnp.where((block_of(source) == near) | (block_of(source) == second), factor * drawn, drawn)


def level_of(key, shape, cuts, low, largest):
    level = 1.0
    for position, blocks in cuts:
        heights = jax.random.uniform(jax.random.fold_in(jax.random.fold_in(key, 6), position), (blocks,), jnp.float32, low / len(cuts), largest / len(cuts))
        level = level * jnp.repeat(jnp.exp(heights), shape[position] // blocks).reshape((-1,) + (1,) * (len(shape) - 1 - position))
    return level


def normal_values(stream_key, dims, scale, limit, split=(), held_as=jnp.bfloat16):
    entries = scale * jax.random.normal(stream_key, dims, jnp.float32)
    if split:
        entries = entries * level_of(stream_key, dims, split, -0.22, 0.18)
    return jnp.clip(entries, -limit, limit).astype(held_as)


def noise_with(stream_key, extent, spread, most, split, heavy, kind=jnp.bfloat16):
    result = spread * jax.random.normal(stream_key, extent, jnp.float32)
    if split:
        result = result * level_of(stream_key, extent, split, -0.22, 0.18)
    return jnp.clip(strengthened(result, jax.random.fold_in(stream_key, 3), *heavy), -most, most).astype(kind)


def setup_inputs(seed: int = 0) -> dict:
    splits = jax.random.split(jax.random.key(seed), 7)
    return {
        "inputs": noise_with(splits[0], (N_SECTION, MB, TOKENS, D), 1.0, 6.0, ((0, 8), (2, 32)), (2, 3, 32, 2.75)),
        "cotangent": normal_values(splits[1], (MB, TOKENS, D), 1.0, 6.0, ((1, 32),)),
        "norm_gain": jnp.clip(1.0 + 0.1 * jax.random.normal(splits[2], (N_SECTION, D), jnp.float32), 0.5, 1.5).astype(jnp.bfloat16),
        "key_weight": normal_values(splits[3], (N_SECTION, D, KV), D ** -0.5, 0.09375, ((0, 8), (1, 32))),
        "value_weight": normal_values(splits[4], (N_SECTION, D, KV), D ** -0.5, 0.09375, ((0, 8), (1, 32))),
        "plan": jax.vmap(lambda own: jax.random.permutation(own, MB))(jax.random.split(splits[5], N_SECTION)).reshape((N_SECTION, MB)).astype(jnp.int32),
    }


eps = 1e-05
rope_base = 500000.0

def rope_tables(length, head_dim):
    half_dim = head_dim // 2
    frequency = rope_base ** (-(jnp.arange(half_dim, dtype=jnp.float32) * 2.0 / head_dim))
    angles = jnp.arange(length, dtype=jnp.float32)[:, None] * frequency[None, :]
    cosine = jnp.concatenate([jnp.cos(angles), jnp.cos(angles)], axis=-1)
    sine_tab = jnp.concatenate([jnp.sin(angles), jnp.sin(angles)], axis=-1)
    return (cosine[:, None, :], sine_tab[:, None, :])

def turned(values):
    half_dim = values.shape[-1] // 2
    return jnp.concatenate([-values[..., half_dim:], values[..., :half_dim]], axis=-1)

def rotate(values, cosine, sine_tab):
    return values * cosine + turned(values) * sine_tab

def unrotate(values, cosine, sine_tab):
    return values * cosine - turned(values) * sine_tab

def forward(x_rows, gain, w_key, w_value):
    batch_count = x_rows.shape[0]
    length = x_rows.shape[1]
    score_scale = 1.0 / math.sqrt(HEAD_DIM)
    widened = x_rows.astype(jnp.float32)
    inv_rms = lax.rsqrt(lax.optimization_barrier(jnp.mean(widened * widened, axis=-1, keepdims=True)) + eps)
    gain_full = gain.astype(jnp.float32)
    normed = (widened * inv_rms * gain_full).astype(jnp.bfloat16)
    flat_normed = normed.reshape(batch_count * length, D)
    key_pre = jnp.dot(flat_normed, w_key, preferred_element_type=jnp.float32).reshape(batch_count, length, KV_HEADS, HEAD_DIM)
    value_heads = jnp.dot(flat_normed, w_value, preferred_element_type=jnp.float32).astype(jnp.bfloat16).reshape(batch_count, length, KV_HEADS, HEAD_DIM)
    cosine, sine_tab = rope_tables(length, HEAD_DIM)
    key_rot = rotate(key_pre, cosine, sine_tab).astype(jnp.bfloat16)
    query_rot = rotate(normed.astype(jnp.float32).reshape(batch_count, length, HEADS, HEAD_DIM), cosine, sine_tab).astype(jnp.bfloat16)
    query_rot = query_rot.reshape(batch_count, length, KV_HEADS, GROUP, HEAD_DIM)
    scores = jnp.einsum('blkgd,bmkd->bkglm', query_rot.astype(jnp.float32), key_rot.astype(jnp.float32)) * score_scale
    causal = jnp.arange(length)[:, None] >= jnp.arange(length)[None, :]
    raised = jnp.where(causal, jnp.exp(scores), 0.0)
    attn_prob = raised / lax.optimization_barrier(jnp.sum(raised, axis=-1, keepdims=True))
    prob_low = attn_prob.astype(jnp.bfloat16)
    return (widened, inv_rms, normed, query_rot, key_rot, value_heads, attn_prob, prob_low)

def backward(upper_grad, widened, inv_rms, normed, query_rot, key_rot, value_heads, attn_prob, prob_low, gain, w_key, w_value):
    batch_count = upper_grad.shape[0]
    length = upper_grad.shape[1]
    score_scale = 1.0 / math.sqrt(HEAD_DIM)
    grad_heads = upper_grad.astype(jnp.float32).reshape(batch_count, length, KV_HEADS, GROUP, HEAD_DIM)
    grad_prob = jnp.einsum('blkgd,bmkd->bkglm', grad_heads, value_heads.astype(jnp.float32))
    grad_value = jnp.einsum('bkglm,blkgd->bmkd', prob_low.astype(jnp.float32), grad_heads).astype(jnp.bfloat16)
    row_dot = lax.optimization_barrier(jnp.sum(attn_prob * grad_prob, axis=-1, keepdims=True))
    grad_score = (attn_prob * (grad_prob - row_dot) * score_scale).astype(jnp.bfloat16)
    grad_query = jnp.einsum('bkglm,bmkd->blkgd', grad_score.astype(jnp.float32), key_rot.astype(jnp.float32))
    grad_key = jnp.einsum('bkglm,blkgd->bmkd', grad_score.astype(jnp.float32), query_rot.astype(jnp.float32))
    cosine, sine_tab = rope_tables(length, HEAD_DIM)
    query_back = unrotate(grad_query.reshape(batch_count, length, HEADS, HEAD_DIM), cosine, sine_tab).reshape(batch_count, length, D)
    key_back = unrotate(grad_key, cosine, sine_tab).astype(jnp.bfloat16).reshape(batch_count * length, KV)
    value_flat = grad_value.reshape(batch_count * length, KV)
    projected_back = jnp.dot(key_back, w_key.T, preferred_element_type=jnp.float32) + jnp.dot(value_flat, w_value.T, preferred_element_type=jnp.float32)
    grad_normed = query_back + projected_back.reshape(batch_count, length, D)
    gain_full = gain.astype(jnp.float32)
    gain_term = grad_normed * widened * inv_rms
    projected = lax.optimization_barrier(jnp.mean(gain_term * gain_full, axis=-1, keepdims=True))
    lower_grad = upper_grad.astype(jnp.float32) + inv_rms * gain_full * grad_normed - widened * inv_rms * inv_rms * projected
    return (lower_grad.astype(jnp.bfloat16), key_back, value_flat, gain_term)

def regroup(array):
    return array.reshape(MB, N_DP, TOK_DEV, -1).transpose(1, 0, 2, 3).reshape(N_DP, MB * TOK_DEV, -1)

def add_group(totals, pieces):
    normed, key_back, value_flat, gain_term = pieces
    sum_key = jnp.dot(normed.T, key_back, preferred_element_type=jnp.float32)
    sum_value = jnp.dot(normed.T, value_flat, preferred_element_type=jnp.float32)
    sum_gain = lax.optimization_barrier(jnp.sum(gain_term, axis=0))
    rounded_key = lax.optimization_barrier(sum_key.astype(jnp.bfloat16)).astype(jnp.float32)
    rounded_value = lax.optimization_barrier(sum_value.astype(jnp.bfloat16)).astype(jnp.float32)
    rounded_gain = lax.optimization_barrier(sum_gain.astype(jnp.bfloat16)).astype(jnp.float32)
    return ((totals[0] + rounded_key, totals[1] + rounded_value, totals[2] + rounded_gain), None)

def reference(inputs, cotangent, norm_gain, key_weight, value_weight, plan):
    upper_grad = cotangent.reshape(MB * N_DP, TOK_DEV, D)
    grad_list = [None] * N_SECTION
    key_list = [None] * N_SECTION
    value_list = [None] * N_SECTION
    gain_list = [None] * N_SECTION
    for section_index in range(N_SECTION - 1, -1, -1):
        x_rows = inputs[section_index].reshape(MB * N_DP, TOK_DEV, D)
        saved = forward(x_rows, norm_gain[section_index], key_weight[section_index], value_weight[section_index])
        lower_grad, key_back, value_flat, gain_term = backward(upper_grad, *saved, norm_gain[section_index], key_weight[section_index], value_weight[section_index])
        normed = saved[2]
        start = (jnp.zeros((D, KV), jnp.float32), jnp.zeros((D, KV), jnp.float32), jnp.zeros((D,), jnp.float32))
        totals, unused = lax.scan(add_group, start, (regroup(normed), regroup(key_back), regroup(value_flat), regroup(gain_term)))
        key_list[section_index] = totals[0]
        value_list[section_index] = totals[1]
        gain_list[section_index] = totals[2]
        blocks = lower_grad.reshape(MB, TOKENS, D)
        grad_list[section_index] = blocks[plan[section_index]]
        upper_grad = lower_grad
    return (jnp.stack(grad_list), jnp.stack(key_list), jnp.stack(value_list), jnp.stack(gain_list))
```

```python
import functools
import math

import jax
import jax.numpy as jnp
import numpy as np
from jax import lax
from jax.experimental import pallas as pl
from jax.experimental.pallas import tpu as pltpu
from jax.sharding import Mesh
from jax.sharding import PartitionSpec as P

MESH_ID = pl.DeviceIdType.MESH
KV_HEADS = 4
GROUP = 8
HEAD_DIM = 128
SECTION = ("y", "xl")
DP = ("xh", "z", "c")
eps = 1e-05
rope_base = 500000.0
VMEM_LIMIT = 60 * 1024 * 1024
F32 = jnp.float32
BF16 = jnp.bfloat16


def rope_tables(length, head_dim):
    half = head_dim // 2
    exponent = -(np.arange(half, dtype=np.float32) * np.float32(2.0) / np.float32(head_dim))
    frequency = np.power(np.float32(rope_base), exponent).astype(np.float32)
    angles = np.arange(length, dtype=np.float32)[:, None] * frequency[None, :]
    cosine, sine = np.cos(angles), np.sin(angles)
    return (
        np.concatenate([cosine, cosine], axis=-1).astype(np.float32),
        np.concatenate([-sine, sine], axis=-1).astype(np.float32),
    )


def greet(peers):
    barrier = pltpu.get_barrier_semaphore()
    for peer in peers:
        pl.semaphore_signal(barrier, inc=1, device_id=peer, device_id_type=MESH_ID)
    pl.semaphore_wait(barrier, len(peers))


def remote(src, dst, send, recv, peer):
    return pltpu.make_async_remote_copy(
        src_ref=src, dst_ref=dst, send_sem=send, recv_sem=recv, device_id=peer, device_id_type=MESH_ID
    )


def nn(a, b):
    return lax.dot_general(a, b, (((1,), (0,)), ((), ())), preferred_element_type=F32)


def nt(a, b):
    return lax.dot_general(a, b, (((1,), (1,)), ((), ())), preferred_element_type=F32)


def tn(a, b):
    return lax.dot_general(a, b, (((0,), (0,)), ((), ())), preferred_element_type=F32)


def gather_kernel(nz, *refs):
    sources, fulls = refs[0:3], refs[3:6]
    xs, xr, zs, zr, ds, dr = refs[6:]
    xh, z, c = lax.axis_index("xh"), lax.axis_index("z"), lax.axis_index("c")
    up, down = lax.rem(z + 1, nz), lax.rem(z + nz - 1, nz)
    across, partner = {"xh": 1 - xh}, {"c": 1 - c}
    toward = ({"z": up}, {"z": down})
    long_way, short_way = nz // 2, nz - 1 - nz // 2
    hops = ((long_way, short_way), (short_way, long_way), (long_way, short_way))
    greet([across, partner, toward[0], toward[1]])
    sends = []

    def push(copy):
        copy.start()
        sends.append(copy)

    def place(p, src, steps):
        row = xh if src == 0 else 1 - xh
        return fulls[p].at[row, lax.rem(z + steps + nz, nz), c]

    def share(p, src, data, slot, index):
        push(remote(data, slot, ds.at[p, src, index], dr.at[p, src, index], partner))

    for p in range(3):
        slot = place(p, 0, 0)
        push(remote(sources[p], slot, xs.at[p], xr.at[p], across))
        for d in range(2):
            push(remote(sources[p], slot, zs.at[d, 0, 0, p], zr.at[d, 0, 0, p], toward[d]))
    for p in range(3):
        share(p, 0, sources[p], place(p, 0, 0), 0)
    for p in range(3):
        fulls[p][xh, z, c] = sources[p][...]
    for p in range(3):
        slot = place(p, 1, 0)
        remote(slot, slot, xs.at[p], xr.at[p], across).wait_recv()
        for d in range(2):
            push(remote(slot, slot, zs.at[d, 0, 1, p], zr.at[d, 0, 1, p], toward[d]))
        share(p, 1, slot, slot, 0)
    for t in range(1, long_way + 1):
        for src in range(2):
            for p in range(3):
                for d in range(2):
                    if t > hops[p][d]:
                        continue
                    slot = place(p, src, -t if d == 0 else t)
                    remote(
                        slot, slot, zs.at[d, t - 1, src, p], zr.at[d, t - 1, src, p], toward[d]
                    ).wait_recv()
                    if t < hops[p][d]:
                        push(remote(slot, slot, zs.at[d, t, src, p], zr.at[d, t, src, p], toward[d]))
                    share(p, src, slot, slot, 1 + 4 * d + t - 1)
    for p in range(3):
        for src in range(2):
            row = xh if src == 0 else 1 - xh
            for d in range(2):
                for t in range(hops[p][d] + 1):
                    if t == 0 and d == 1:
                        continue
                    index = 0 if t == 0 else 1 + 4 * d + t - 1
                    steps = -t if d == 0 else t
                    slot = fulls[p].at[row, lax.rem(z + steps + nz, nz), 1 - c]
                    remote(slot, slot, ds.at[p, src, index], dr.at[p, src, index], partner).wait_recv()
    for copy in sends:
        copy.wait_send()


def gather_weights(key_weight, value_weight, gain, nxh, nz, nc):
    sources = (key_weight, value_weight, gain)
    return pl.pallas_call(
        functools.partial(gather_kernel, nz),
        out_shape=[jax.ShapeDtypeStruct((nxh, nz, nc, *a.shape), a.dtype) for a in sources],
        in_specs=[pl.BlockSpec(memory_space=pltpu.VMEM)] * 3,
        out_specs=[pl.BlockSpec(memory_space=pltpu.VMEM)] * 3,
        scratch_shapes=[
            pltpu.SemaphoreType.DMA((3,)),
            pltpu.SemaphoreType.DMA((3,)),
            pltpu.SemaphoreType.DMA((2, 4, 2, 3)),
            pltpu.SemaphoreType.DMA((2, 4, 2, 3)),
            pltpu.SemaphoreType.DMA((3, 2, 9)),
            pltpu.SemaphoreType.DMA((3, 2, 9)),
        ],
        compiler_params=pltpu.CompilerParams(
            collective_id=0, has_side_effects=True, vmem_limit_bytes=VMEM_LIMIT
        ),
        name="gather_weights",
    )(*sources)


def relay_kernel(
    ny, nz, x_ref, cot_ref, wk_ref, wv_ref, gain_ref, cos_ref, sin_ref,
    low_ref, rows_ref, kv_ref, colsum_ref,
    up_ref, normed_s, out_rows, key_s, value_s, query_s, prob_s, inv_s, qb_s, gsum_s,
    us, ur, ns, nr,
):
    y, xl = lax.axis_index("y"), lax.axis_index("xl")
    xh, c = lax.axis_index("xh"), lax.axis_index("c")
    section, sections = y * 2 + xl, ny * 2
    batches, tokens, width = x_ref.shape
    kv_width = wk_ref.shape[1]
    block = GROUP * HEAD_DIM
    scale = 1.0 / math.sqrt(HEAD_DIM)
    below = lax.rem(section + sections - 1, sections)
    above = lax.rem(section + 1, sections)
    lower_peer = {"y": below // 2, "xl": lax.rem(below, 2)}
    upper_peer = {"y": above // 2, "xl": lax.rem(above, 2)}
    near = ((xh, 1 - c), (1 - xh, c), (1 - xh, 1 - c))
    row_peers = [{"xh": a, "c": b} for a, b in near]
    greet([lower_peer, upper_peer] + row_peers)
    cosine, sine = cos_ref[...], sin_ref[...]

    def rotate(v):
        return v * cosine + pltpu.roll(v, HEAD_DIM // 2, axis=1) * sine

    def unrotate(v):
        return v * cosine - pltpu.roll(v, HEAD_DIM // 2, axis=1) * sine

    def head(h):
        return slice(h * HEAD_DIM, (h + 1) * HEAD_DIM)

    gsum_s[...] = jnp.zeros_like(gsum_s)
    for i in range(batches):
        here = slice(i * tokens, (i + 1) * tokens)
        total = jnp.zeros((tokens, HEAD_DIM), F32)
        for h in range(width // HEAD_DIM):
            piece = x_ref[i, :, head(h)].astype(F32)
            total = total + piece * piece
        inv = lax.rsqrt(jnp.sum(total, axis=-1, keepdims=True) * (1.0 / width) + eps)
        inv_s[here, :] = jnp.broadcast_to(inv, (tokens, HEAD_DIM))
        for h in range(width // HEAD_DIM):
            piece = x_ref[i, :, head(h)].astype(F32)
            normed = (piece * inv * gain_ref[:, head(h)]).astype(BF16)
            normed_s[here, head(h)] = normed
            a, zz, b = h // (2 * nz), (h // 2) % nz, h % 2
            out_rows[a, b, here, head(zz)] = normed
            rot = rotate(normed.astype(F32)).astype(BF16)
            query_s[i, h // GROUP, slice((h % GROUP) * tokens, (h % GROUP + 1) * tokens), :] = rot
    rows_ref[xh, c] = out_rows[xh, c]
    row_sends = []
    for n, (a, b) in enumerate(near):
        copy = remote(out_rows.at[a, b], rows_ref.at[xh, c], ns.at[n], nr.at[n], row_peers[n])
        copy.start()
        row_sends.append(copy)
    key_pre = nn(normed_s[...], wk_ref[...])
    value_pre = nn(normed_s[...], wv_ref[...])
    for i in range(batches):
        here = slice(i * tokens, (i + 1) * tokens)
        for k in range(KV_HEADS):
            key_s[i, k] = rotate(key_pre[here, head(k)]).astype(BF16)
            value_s[i, k] = value_pre[here, head(k)].astype(BF16)
    m_at = lax.broadcasted_iota(jnp.int32, (tokens, GROUP * tokens), 0)
    l_at = lax.rem(lax.broadcasted_iota(jnp.int32, (tokens, GROUP * tokens), 1), tokens)
    causal = m_at <= l_at
    for i in range(batches):
        for k in range(KV_HEADS):
            scores = nt(key_s[i, k], query_s[i, k]) * scale
            raised = jnp.where(causal, jnp.exp(scores), 0.0)
            prob_s[i, k] = raised / jnp.sum(raised, axis=0, keepdims=True)

    @pl.when(section == sections - 1)
    def _():
        up_ref[...] = cot_ref[...]

    def chunk(ref, i, k):
        return ref.at[i, :, pl.ds(k * block, block)]

    def outgoing(i, k):
        return remote(chunk(low_ref, i, k), chunk(up_ref, i, k), us.at[i, k], ur.at[i, k], lower_peer)

    def one_batch(i, carry):
        start = pl.multiple_of(i * tokens, tokens)
        here = pl.ds(start, tokens)
        for k in range(KV_HEADS):

            @pl.when(section < sections - 1)
            def _():
                remote(
                    chunk(low_ref, i, k), chunk(up_ref, i, k), us.at[i, k], ur.at[i, k], lower_peer
                ).wait_recv()

            upper = jnp.concatenate(
                [up_ref[i, :, head(k * GROUP + h)] for h in range(GROUP)], axis=0
            )
            prob = prob_s[i, k]
            grad_prob = nt(value_s[i, k], upper)
            grad_value = nn(prob.astype(BF16), upper).astype(BF16)
            row_dot = jnp.sum(prob * grad_prob, axis=0, keepdims=True)
            grad_score = (prob * (grad_prob - row_dot) * scale).astype(BF16)
            grad_query = tn(grad_score, key_s[i, k])
            grad_key = nn(grad_score, query_s[i, k])
            kv_ref[here, head(k)] = unrotate(grad_key).astype(BF16)
            kv_ref[here, slice(kv_width + k * HEAD_DIM, kv_width + (k + 1) * HEAD_DIM)] = grad_value
            for h in range(GROUP):
                qb_s[:, head(k * GROUP + h)] = unrotate(
                    grad_query[h * tokens : (h + 1) * tokens, :]
                )
        key_back = kv_ref[here, 0:kv_width]
        value_flat = kv_ref[here, kv_width : 2 * kv_width]
        inv = inv_s[here, :][:, 0:1]
        mean = jnp.zeros((tokens, HEAD_DIM), F32)
        for k in range(KV_HEADS):
            cols = slice(k * block, (k + 1) * block)
            projected = nt(key_back, wk_ref[cols, :]) + nt(value_flat, wv_ref[cols, :])
            for h in range(GROUP):
                at = head(k * GROUP + h)
                grad_normed = qb_s[:, at] + projected[:, head(h)]
                qb_s[:, at] = grad_normed
                term = grad_normed * x_ref[i, :, at].astype(F32) * inv
                gsum_s[:, at] += jnp.sum(term.reshape(tokens // 8, 8, HEAD_DIM), axis=0)
                mean = mean + term * gain_ref[:, at]
        row_mean = jnp.sum(mean, axis=-1, keepdims=True) * (1.0 / width)
        drop = inv * inv * row_mean
        for k in range(KV_HEADS):
            for h in range(GROUP):
                at = head(k * GROUP + h)
                low_ref[i, :, at] = (
                    up_ref[i, :, at].astype(F32)
                    + inv * gain_ref[:, at] * qb_s[:, at]
                    - x_ref[i, :, at].astype(F32) * drop
                ).astype(BF16)

            @pl.when(section > 0)
            def _():
                outgoing(i, k).start()

        return carry

    lax.fori_loop(0, batches, one_batch, 0)
    column = jnp.sum(gsum_s[...], axis=0, keepdims=True)
    pieces = []
    for a in range(2):
        for b in range(2):
            pieces.append(
                jnp.concatenate(
                    [column[:, head(a * 2 * nz + 2 * zz + b)] for zz in range(nz)], axis=1
                )
            )
    pieces.append(jnp.zeros((12, nz * HEAD_DIM), F32))
    colsum_ref[...] = jnp.concatenate(pieces, axis=0).astype(BF16)
    for n, (a, b) in enumerate(near):
        remote(out_rows.at[a, b], rows_ref.at[a, b], ns.at[n], nr.at[n], row_peers[n]).wait_recv()
    for copy in row_sends:
        copy.wait_send()

    @pl.when(section > 0)
    def _():
        for i in range(batches):
            for k in range(KV_HEADS):
                outgoing(i, k).wait_send()


def relay(x, cot, wk, wv, gain, ny, nz):
    batches, tokens, width = x.shape
    kv_width = wk.shape[1]
    cosine, sine = rope_tables(tokens, HEAD_DIM)
    rows = batches * tokens
    return pl.pallas_call(
        functools.partial(relay_kernel, ny, nz),
        out_shape=[
            jax.ShapeDtypeStruct((batches, tokens, width), BF16),
            jax.ShapeDtypeStruct((2, 2, rows, nz * HEAD_DIM), BF16),
            jax.ShapeDtypeStruct((rows, 2 * kv_width), BF16),
            jax.ShapeDtypeStruct((16, nz * HEAD_DIM), BF16),
        ],
        in_specs=[pl.BlockSpec(memory_space=pltpu.VMEM)] * 7,
        out_specs=[pl.BlockSpec(memory_space=pltpu.VMEM)] * 4,
        scratch_shapes=[
            pltpu.VMEM((batches, tokens, width), BF16),
            pltpu.VMEM((rows, width), BF16),
            pltpu.VMEM((2, 2, rows, nz * HEAD_DIM), BF16),
            pltpu.VMEM((batches, KV_HEADS, tokens, HEAD_DIM), BF16),
            pltpu.VMEM((batches, KV_HEADS, tokens, HEAD_DIM), BF16),
            pltpu.VMEM((batches, KV_HEADS, GROUP * tokens, HEAD_DIM), BF16),
            pltpu.VMEM((batches, KV_HEADS, tokens, GROUP * tokens), F32),
            pltpu.VMEM((rows, HEAD_DIM), F32),
            pltpu.VMEM((tokens, width), F32),
            pltpu.VMEM((8, width), F32),
            pltpu.SemaphoreType.DMA((batches, KV_HEADS)),
            pltpu.SemaphoreType.DMA((batches, KV_HEADS)),
            pltpu.SemaphoreType.DMA((3,)),
            pltpu.SemaphoreType.DMA((3,)),
        ],
        compiler_params=pltpu.CompilerParams(
            collective_id=1, has_side_effects=True, vmem_limit_bytes=VMEM_LIMIT
        ),
        name="relay",
    )(x, cot, wk, wv, gain, jnp.asarray(cosine), jnp.asarray(sine))


SUBS = 2


def reduce_kernel(
    nz, rows_ref, kv_ref, colsum_ref, key_out, value_out, gain_out,
    kv_all, col_all, sbuf, rbuf, gsend, grecv, ks, kr, cs, cr, zs, zr, gs, gr,
):
    xh, z, c = lax.axis_index("xh"), lax.axis_index("z"), lax.axis_index("c")
    across, partner = {"xh": 1 - xh}, {"c": 1 - c}
    toward = ({"z": lax.rem(z + 1, nz)}, {"z": lax.rem(z + nz - 1, nz)})
    ring = [{"z": lax.rem(z + s, nz)} for s in range(1, nz)]
    greet([across, partner] + ring)
    kv_width = key_out.shape[1]
    depth = key_out.shape[0]
    part = depth // SUBS
    sends = []

    def push(copy):
        copy.start()
        sends.append(copy)

    for n, peer in enumerate((partner, across)):
        push(remote(kv_ref, kv_all.at[xh, c], ks.at[n], kr.at[n], peer))
        push(remote(colsum_ref, col_all.at[xh, c], cs.at[n], cr.at[n], peer))
    kv_all[xh, c] = kv_ref[...]
    col_all[xh, c] = colsum_ref[...]
    slot, cslot = kv_all.at[1 - xh, c], col_all.at[1 - xh, c]
    remote(slot, slot, ks.at[1], kr.at[1], across).wait_recv()
    push(remote(slot, slot, ks.at[2], kr.at[2], partner))
    remote(cslot, cslot, cs.at[1], cr.at[1], across).wait_recv()
    push(remote(cslot, cslot, cs.at[2], cr.at[2], partner))
    for n, a in ((0, xh), (2, 1 - xh)):
        slot, cslot = kv_all.at[a, 1 - c], col_all.at[a, 1 - c]
        remote(slot, slot, ks.at[n], kr.at[n], partner).wait_recv()
        remote(cslot, cslot, cs.at[n], cr.at[n], partner).wait_recv()

    def partial(target, p):
        at = pl.ds(pl.multiple_of(target * HEAD_DIM, HEAD_DIM), HEAD_DIM)
        total = None
        for a in range(2):
            for b in range(2):
                one = tn(rows_ref[a, b, :, at], kv_all[a, b, :, p * kv_width : (p + 1) * kv_width])
                total = one if total is None else total + one
        return total

    long_way, short_way = nz // 2, nz - 1 - nz // 2
    hops = ((long_way, short_way), (short_way, long_way))

    def ring_copy(d, p, t, s):
        return remote(
            sbuf.at[d, p, t, s], rbuf.at[d, p, t, s], zs.at[d, p, t, s], zr.at[d, p, t, s], toward[d]
        )

    for t in range(long_way):
        for p in range(2):
            for d in range(2):
                if t >= hops[p][d]:
                    continue
                steps = hops[p][d] - t
                target = lax.rem(z + (steps if d == 0 else nz - steps), nz)
                mine = partial(target, p)
                for s in range(SUBS):
                    piece = mine[s * part : (s + 1) * part, :]
                    if t > 0:
                        ring_copy(d, p, t - 1, s).wait_recv()
                        piece = piece + rbuf[d, p, t - 1, s].astype(F32)
                    sbuf[d, p, t, s] = piece.astype(BF16)
                    push(ring_copy(d, p, t, s))
        if t == 0:
            own = lax.broadcasted_iota(jnp.int32, (16, nz * HEAD_DIM), 0) == xh * 2 + c
            totals = jnp.zeros((16, nz * HEAD_DIM), F32)
            for a in range(2):
                for b in range(2):
                    totals = totals + col_all[a, b].astype(F32)
            line = jnp.sum(jnp.where(own, totals, 0.0), axis=0, keepdims=True)
            for zz in range(nz):
                gsend[zz] = jnp.broadcast_to(
                    line[:, zz * HEAD_DIM : (zz + 1) * HEAD_DIM], (8, HEAD_DIM)
                )
            for s in range(1, nz):
                push(
                    remote(
                        gsend.at[lax.rem(z + s, nz)], grecv.at[s - 1], gs.at[s - 1], gr.at[s - 1],
                        ring[s - 1],
                    )
                )
    outs = (key_out, value_out)
    for p in range(2):
        mine = partial(z, p)
        for s in range(SUBS):
            piece = mine[s * part : (s + 1) * part, :]
            for d in range(2):
                last = hops[p][d] - 1
                ring_copy(d, p, last, s).wait_recv()
                piece = piece + rbuf[d, p, last, s].astype(F32)
            outs[p][s * part : (s + 1) * part, :] = piece
    column = gsend[z]
    for s in range(1, nz):
        remote(
            gsend.at[0], grecv.at[s - 1], gs.at[s - 1], gr.at[s - 1], ring[s - 1]
        ).wait_recv()
        column = column + grecv[s - 1]
    gain_out[...] = column
    for copy in sends:
        copy.wait_send()


def reduce_weights(rows, kv, colsum, nz):
    total_rows, both = kv.shape
    half = both // 2
    ring = (2, 2, nz // 2, SUBS)
    return pl.pallas_call(
        functools.partial(reduce_kernel, nz),
        out_shape=[
            jax.ShapeDtypeStruct((HEAD_DIM, half), F32),
            jax.ShapeDtypeStruct((HEAD_DIM, half), F32),
            jax.ShapeDtypeStruct((8, HEAD_DIM), F32),
        ],
        in_specs=[pl.BlockSpec(memory_space=pltpu.VMEM)] * 3,
        out_specs=[pl.BlockSpec(memory_space=pltpu.VMEM)] * 3,
        scratch_shapes=[
            pltpu.VMEM((2, 2, total_rows, both), BF16),
            pltpu.VMEM((2, 2, 16, colsum.shape[1]), BF16),
            pltpu.VMEM((*ring, HEAD_DIM // SUBS, half), BF16),
            pltpu.VMEM((*ring, HEAD_DIM // SUBS, half), BF16),
            pltpu.VMEM((nz, 8, HEAD_DIM), F32),
            pltpu.VMEM((nz - 1, 8, HEAD_DIM), F32),
            pltpu.SemaphoreType.DMA((3,)),
            pltpu.SemaphoreType.DMA((3,)),
            pltpu.SemaphoreType.DMA((3,)),
            pltpu.SemaphoreType.DMA((3,)),
            pltpu.SemaphoreType.DMA(ring),
            pltpu.SemaphoreType.DMA(ring),
            pltpu.SemaphoreType.DMA((nz - 1,)),
            pltpu.SemaphoreType.DMA((nz - 1,)),
        ],
        compiler_params=pltpu.CompilerParams(
            collective_id=2, has_side_effects=True, vmem_limit_bytes=VMEM_LIMIT
        ),
        name="reduce_weights",
    )(rows, kv, colsum)


def solution(mesh):
    sections, dp = mesh.shape["section"], mesh.shape["dp"]
    ny, nz = sections // 2, dp // 4
    split = Mesh(mesh.devices.reshape(ny, 2, 2, nz, 2), ("y", "xl", "xh", "z", "c"))

    def body(inputs, cotangent, norm_gain, key_weight, value_weight, plan):
        _, batches, tokens, width = inputs.shape
        kv_width = key_weight.shape[2]
        own_gain = jnp.broadcast_to(norm_gain[0].astype(F32)[None, :], (8, HEAD_DIM))
        wk, wv, gains = gather_weights(key_weight[0], value_weight[0], own_gain, 2, nz, 2)
        wk, wv = wk.reshape(width, kv_width), wv.reshape(width, kv_width)
        gain = gains[:, :, :, 0, :].reshape(1, width)
        low, rows, kv, colsum = relay(inputs[0], cotangent, wk, wv, gain, ny, nz)
        key_grad, value_grad, gain_grad = reduce_weights(rows, kv, colsum, nz)
        selector = plan[0][:, None] == jnp.arange(batches, dtype=jnp.int32)[None, :]
        ordered = jnp.sum(
            jnp.where(selector[:, :, None, None], low[None], jnp.zeros((), BF16)), axis=1
        )
        return ordered[None], key_grad[None], value_grad[None], gain_grad[0:1]

    placed = (
        P(SECTION, None, DP, None),
        P(None, DP, None),
        P(SECTION, DP),
        P(SECTION, DP, None),
        P(SECTION, DP, None),
        P(SECTION, None),
    )
    return jax.shard_map(
        body,
        mesh=split,
        in_specs=placed,
        out_specs=(
            P(SECTION, None, DP, None),
            P(SECTION, DP, None),
            P(SECTION, DP, None),
            P(SECTION, DP),
        ),
        check_vma=False,
    )
```

```python
import functools
import math

import jax
import jax.numpy as jnp
import numpy as np
from jax import lax
from jax.experimental import pallas as pl
from jax.experimental.pallas import tpu as pltpu
from jax.sharding import Mesh
from jax.sharding import PartitionSpec as P

MESH_ID = pl.DeviceIdType.MESH
KV_HEADS = 4
GROUP = 8
HEAD_DIM = 128
SECTION = ("y", "xl")
DP = ("xh", "z", "c")
eps = 1e-05
rope_base = 500000.0
VMEM_LIMIT = 60 * 1024 * 1024
F32 = jnp.float32
BF16 = jnp.bfloat16

PIECES = 8
DETOUR = (0, 1, 2)
SEND_ORDER = (0, 4, 1, 5, 2, 6, 7, 3)
KEY_ORDER = (2, 3, 0, 1)
SUBS = 2


def rope_tables(length, head_dim):
    half = head_dim // 2
    exponent = -(np.arange(half, dtype=np.float32) * np.float32(2.0) / np.float32(head_dim))
    frequency = np.power(np.float32(rope_base), exponent).astype(np.float32)
    angles = np.arange(length, dtype=np.float32)[:, None] * frequency[None, :]
    cosine, sine = np.cos(angles), np.sin(angles)
    return (
        np.concatenate([cosine, cosine], axis=-1).astype(np.float32),
        np.concatenate([-sine, sine], axis=-1).astype(np.float32),
    )


def remote(src, dst, send, recv, peer):
    return pltpu.make_async_remote_copy(
        src_ref=src, dst_ref=dst, send_sem=send, recv_sem=recv, device_id=peer, device_id_type=MESH_ID
    )


def nn(a, b):
    return lax.dot_general(a, b, (((1,), (0,)), ((), ())), preferred_element_type=F32)


def nt(a, b):
    return lax.dot_general(a, b, (((1,), (1,)), ((), ())), preferred_element_type=F32)


def tn(a, b):
    return lax.dot_general(a, b, (((0,), (0,)), ((), ())), preferred_element_type=F32)


def head(h):
    return slice(h * HEAD_DIM, (h + 1) * HEAD_DIM)


def kernel(
    ny, nz,
    x_ref, cot_ref, wk_ref, wv_ref, gain_ref, plan_ref, cos_ref, sin_ref,
    low_out, key_out, value_out, gain_out,
    fk, fv, fg, up_ref, low_s, via_ref, normed_s, out_rows, rows_all, key_s, value_s, query_s,
    prob_s, inv_s, qb_s, pre_k, pre_v, kv_s, kv_all, col_s, col_all, sbuf, rbuf, gsend, grecv,
    xs, xr, zs, zr, ws, wr, ds, dr,
    us, ur, vs, vr, fs, ns, nr, ks, kr, cs, cr, rs, rr, gs, gr,
):
    y, xl = lax.axis_index("y"), lax.axis_index("xl")
    xh, z, c = lax.axis_index("xh"), lax.axis_index("z"), lax.axis_index("c")
    section, sections = y * 2 + xl, ny * 2
    batches, tokens, width = x_ref.shape
    kv_width = wk_ref.shape[1]
    heads = width // HEAD_DIM
    scale = 1.0 / math.sqrt(HEAD_DIM)

    def section_peer(steps):
        there = lax.rem(section + sections + steps, sections)
        return {"y": there // 2, "xl": lax.rem(there, 2)}

    below, above = section_peer(-1), section_peer(1)
    two_below, two_above = section_peer(-2), section_peer(2)
    across, partner, corner = {"xh": 1 - xh}, {"c": 1 - c}, {"xh": 1 - xh, "c": 1 - c}
    ring = [{"z": lax.rem(z + s, nz)} for s in range(1, nz)]
    toward = (ring[0], ring[nz - 2])
    long_way, short_way = nz // 2, nz - 1 - nz // 2

    barrier = pltpu.get_barrier_semaphore()
    greeted = [across, partner, corner, below, above, two_below, two_above] + ring
    for peer in greeted:
        pl.semaphore_signal(barrier, inc=1, device_id=peer, device_id_type=MESH_ID)
    pl.semaphore_wait(barrier, len(greeted))

    sends = []

    def push(copy):
        copy.start()
        sends.append(copy)

    cosine, sine = cos_ref[...], sin_ref[...]

    def rotate(v):
        return v * cosine + pltpu.roll(v, HEAD_DIM // 2, axis=1) * sine

    def unrotate(v):
        return v * cosine - pltpu.roll(v, HEAD_DIM // 2, axis=1) * sine

    def gain(h):
        return fg[h // (2 * nz), (h // 2) % nz, h % 2, 0:1, :]

    sources, fulls = (wk_ref, wv_ref, gain_ref), (fk, fv, fg)
    hops = ((long_way, short_way), (short_way, long_way), (long_way, short_way))

    def place(p, src, steps, core=c):
        row = xh if src == 0 else 1 - xh
        return fulls[p].at[row, lax.rem(z + steps + nz, nz), core]

    def index_of(d, t):
        return 0 if t == 0 else 1 + long_way * d + t - 1

    def steps_of(d, t):
        return -t if d == 0 else t

    def share(p, src, data, slot, index):
        push(remote(data, slot, ds.at[p, src, index], dr.at[p, src, index], partner))

    def ring_copy(data, slot, d, t, src, p):
        return remote(data, slot, zs.at[d, t, src, p], zr.at[d, t, src, p], toward[d])

    def first_moves(p):
        slot = place(p, 0, 0)
        if p != 1:
            push(remote(sources[p], slot, xs.at[p], xr.at[p], across))
        else:
            push(remote(sources[p], slot, ws.at[0], wr.at[0], across))
        for d in range(2):
            push(ring_copy(sources[p], slot, d, 0, 0, p))
        share(p, 0, sources[p], slot, 0)
        fulls[p][xh, z, c] = sources[p][...]

    def row_arrival(p):
        slot = place(p, 1, 0)
        remote(slot, slot, xs.at[p], xr.at[p], across).wait_recv()
        for d in range(2):
            push(ring_copy(slot, slot, d, 0, 1, p))
        share(p, 1, slot, slot, 0)

    def ring_arrival(p, src, d, t):
        if t > hops[p][d]:
            return
        slot = place(p, src, steps_of(d, t))
        ring_copy(slot, slot, d, t - 1, src, p).wait_recv()
        if t < hops[p][d]:
            push(ring_copy(slot, slot, d, t, src, p))
        index = index_of(d, t)
        if p == 1:
            push(remote(slot, slot, ws.at[index], wr.at[index], across))
        share(p, src, slot, slot, index)

    def cross_arrival(d, t):
        if t > hops[1][d]:
            return
        index = index_of(d, t)
        slot = place(1, 1, steps_of(d, t))
        remote(slot, slot, ws.at[index], wr.at[index], across).wait_recv()
        share(1, 1, slot, slot, index)

    def shared_arrivals(p):
        for src in range(2):
            for d in range(2):
                for t in range(hops[p][d] + 1):
                    if t == 0 and d == 1:
                        continue
                    index = index_of(d, t)
                    slot = place(p, src, steps_of(d, t), 1 - c)
                    remote(slot, slot, ds.at[p, src, index], dr.at[p, src, index], partner).wait_recv()

    def mean_square(i):
        here = slice(i * tokens, (i + 1) * tokens)
        total = jnp.zeros((tokens, HEAD_DIM), F32)
        for h in range(heads):
            piece = x_ref[i, :, head(h)].astype(F32)
            total = total + piece * piece
        inv = lax.rsqrt(jnp.sum(total, axis=-1, keepdims=True) * (1.0 / width) + eps)
        inv_s[here, :] = jnp.broadcast_to(inv, (tokens, HEAD_DIM))

    def normalise(i, h):
        here = slice(i * tokens, (i + 1) * tokens)
        piece = x_ref[i, :, head(h)].astype(F32)
        normed = (piece * inv_s[here, :] * gain(h)).astype(BF16)
        normed_s[here, head(h)] = normed
        out_rows[h // (2 * nz), h % 2, here, head((h // 2) % nz)] = normed
        rows = slice((h % GROUP) * tokens, (h % GROUP + 1) * tokens)
        query_s[i, h // GROUP, rows, :] = rotate(normed.astype(F32)).astype(BF16)

    first_moves(2)
    first_moves(0)
    first_moves(1)
    mean_square(0)
    row_arrival(2)
    for t in range(1, long_way + 1):
        for src in range(2):
            for d in range(2):
                ring_arrival(2, src, d, t)
        if t == 1:
            row_arrival(0)
            mean_square(1)
    shared_arrivals(2)
    waiting = [(i, h) for i in range(batches) for h in range(heads)]
    share_of = -(-len(waiting) // (2 * long_way))

    def some_work():
        for _ in range(min(share_of, len(waiting))):
            normalise(*waiting.pop(0))

    for t in range(1, long_way + 1):
        for d in range(2):
            ring_arrival(0, 0, d, t)
            ring_arrival(1, 0, d, t)
        some_work()
        for d in range(2):
            ring_arrival(0, 1, d, t)
            if t > 1 or d == 0:
                cross_arrival(d, t - 1)
        some_work()
    while waiting:
        some_work()
    for d in range(2):
        cross_arrival(d, long_way)
    shared_arrivals(0)
    shared_arrivals(1)
    wk, wv = fk.reshape(width, kv_width), fv.reshape(width, kv_width)

    near = ((xh, 1 - c), (1 - xh, c), (1 - xh, 1 - c))
    row_peers = (partner, across, corner)

    def row_copy(n):
        return remote(
            out_rows.at[near[n][0], near[n][1]], rows_all.at[xh, c], ns.at[n], nr.at[n], row_peers[n]
        )

    rows_all[xh, c] = out_rows[xh, c]

    @pl.when(section < sections - 2)
    def _():
        for n in range(3):
            row_copy(n).start()

    key_pre = nn(normed_s[...], wk[...])
    value_pre = nn(normed_s[...], wv[...])
    pre_k[...] = key_pre
    pre_v[...] = value_pre
    m_at = lax.broadcasted_iota(jnp.int32, (tokens, GROUP * tokens), 0)
    l_at = lax.rem(lax.broadcasted_iota(jnp.int32, (tokens, GROUP * tokens), 1), tokens)
    causal = m_at <= l_at
    for i in range(batches):
        here = slice(i * tokens, (i + 1) * tokens)
        for k in range(KV_HEADS):
            key_s[i, k] = rotate(key_pre[here, head(k)]).astype(BF16)
            value_s[i, k] = value_pre[here, head(k)].astype(BF16)
            scores = nt(key_s[i, k], query_s[i, k]) * scale
            raised = jnp.where(causal, jnp.exp(scores), 0.0)
            prob_s[i, k] = raised / jnp.sum(raised, axis=0, keepdims=True)

    piece_width = width // PIECES
    piece_heads = heads // PIECES

    @pl.when(section == sections - 1)
    def _():
        up_ref[...] = cot_ref[...]

    def piece(ref, i, j):
        return ref.at[i, :, pl.ds(j * piece_width, piece_width)]

    def outgoing(i, j):
        if j in DETOUR:
            n = DETOUR.index(j)
            return remote(piece(low_s, i, j), via_ref.at[i, n], us.at[i, j], vr.at[i, n], two_below)
        return remote(piece(low_s, i, j), piece(up_ref, i, j), us.at[i, j], ur.at[i, j], below)

    def onward(i, n):
        return remote(
            via_ref.at[i, n], piece(up_ref, i, DETOUR[n]), fs.at[i, n], ur.at[i, DETOUR[n]], above
        )

    def pass_on(i):
        for n in range(len(DETOUR)):
            remote(via_ref.at[i, n], via_ref.at[i, n], fs.at[i, n], vr.at[i, n], above).wait_recv()
            onward(i, n).start()

    def kv_copy(i, n):
        peer = (partner, across)[n]
        return remote(kv_s.at[i], kv_all.at[xh, c, i], ks.at[i, n], kr.at[i, n], peer)

    @pl.when(section < sections - 2)
    def _():
        for i in range(batches):
            pass_on(i)

    def one_batch(i, carry):
        start = pl.multiple_of(i * tokens, tokens)
        here = pl.ds(start, tokens)
        inv = inv_s[here, :]
        mean = jnp.zeros((tokens, HEAD_DIM), F32)
        for k in KEY_ORDER:

            @pl.when(section < sections - 1)
            def _():
                for j in (2 * k, 2 * k + 1):
                    slot = piece(up_ref, i, j)
                    remote(slot, slot, us.at[i, j], ur.at[i, j], below).wait_recv()

            upper = jnp.concatenate(
                [up_ref[i, :, head(k * GROUP + h)] for h in range(GROUP)], axis=0
            )
            prob = prob_s[i, k]
            grad_prob = nt(value_s[i, k], upper)
            grad_value = nn(prob.astype(BF16), upper).astype(BF16)
            row_dot = jnp.sum(prob * grad_prob, axis=0, keepdims=True)
            grad_score = (prob * (grad_prob - row_dot) * scale).astype(BF16)
            grad_query = tn(grad_score, key_s[i, k])
            key_back = unrotate(nn(grad_score, query_s[i, k])).astype(BF16)
            kv_s[i, :, head(k)] = key_back
            kv_s[i, :, head(KV_HEADS + k)] = grad_value
            mean = mean + key_back.astype(F32) * pre_k[here, head(k)]
            mean = mean + grad_value.astype(F32) * pre_v[here, head(k)]
            for h in range(GROUP):
                at = head(k * GROUP + h)
                query_back = unrotate(grad_query[h * tokens : (h + 1) * tokens, :])
                qb_s[i, :, at] = query_back
                mean = mean + query_back * (
                    x_ref[i, :, at].astype(F32) * inv * gain(k * GROUP + h)
                )
        row_mean = jnp.sum(mean, axis=-1, keepdims=True) * (1.0 / width)
        drop = inv * inv * row_mean
        key_flat = kv_s[i, :, 0:kv_width]
        value_flat = kv_s[i, :, kv_width : 2 * kv_width]
        for j in SEND_ORDER:
            cols = slice(j * piece_width, (j + 1) * piece_width)
            projected = nt(key_flat, wk[cols, :]) + nt(value_flat, wv[cols, :])
            for h in range(piece_heads):
                at = head(j * piece_heads + h)
                grad_normed = qb_s[i, :, at] + projected[:, head(h)]
                qb_s[i, :, at] = grad_normed
                low_s[i, :, at] = (
                    up_ref[i, :, at].astype(F32)
                    + inv * gain(j * piece_heads + h) * grad_normed
                    - x_ref[i, :, at].astype(F32) * drop
                ).astype(BF16)

            @pl.when(section > 0)
            def _():
                outgoing(i, j).start()

        @pl.when(section == 0)
        def _():
            for n in range(2):
                kv_copy(i, n).start()

        return carry

    lax.fori_loop(0, batches, one_batch, 0)

    @pl.when(section > 0)
    def _():
        for i in range(batches):
            for n in range(2):
                kv_copy(i, n).start()

    @pl.when(section >= sections - 2)
    def _():
        for n in range(3):
            row_copy(n).start()

    @pl.when(section == sections - 1)
    def _():
        for i in range(batches):
            pass_on(i)

    columns = []
    for h in range(heads):
        at = head(h)
        total = jnp.zeros((8, HEAD_DIM), F32)
        for i in range(batches):
            here = slice(i * tokens, (i + 1) * tokens)
            term = qb_s[i, :, at] * x_ref[i, :, at].astype(F32) * inv_s[here, :]
            total = total + jnp.sum(term.reshape(tokens // 8, 8, HEAD_DIM), axis=0)
        columns.append(jnp.sum(total, axis=0, keepdims=True))
    lines = [
        jnp.concatenate([columns[a * 2 * nz + 2 * zz + b] for zz in range(nz)], axis=1)
        for a in range(2)
        for b in range(2)
    ]
    lines.append(jnp.zeros((12, nz * HEAD_DIM), F32))
    col_s[...] = jnp.concatenate(lines, axis=0).astype(BF16)
    kv_all[xh, c] = kv_s[...]
    col_all[xh, c] = col_s[...]
    for n, peer in enumerate((partner, across)):
        push(remote(col_s, col_all.at[xh, c], cs.at[n], cr.at[n], peer))
    for i in range(batches):
        slot = kv_all.at[1 - xh, c, i]
        remote(slot, slot, ks.at[i, 1], kr.at[i, 1], across).wait_recv()
        push(remote(slot, slot, ks.at[i, 2], kr.at[i, 2], partner))
    slot = col_all.at[1 - xh, c]
    remote(slot, slot, cs.at[1], cr.at[1], across).wait_recv()
    push(remote(slot, slot, cs.at[2], cr.at[2], partner))
    for n in range(3):
        slot = rows_all.at[near[n][0], near[n][1]]
        remote(slot, slot, ns.at[n], nr.at[n], row_peers[n]).wait_recv()
    for n, a in ((0, xh), (2, 1 - xh)):
        for i in range(batches):
            slot = kv_all.at[a, 1 - c, i]
            remote(slot, slot, ks.at[i, n], kr.at[i, n], partner).wait_recv()
        slot = col_all.at[a, 1 - c]
        remote(slot, slot, cs.at[n], cr.at[n], partner).wait_recv()

    total_rows = 4 * batches * tokens

    def partial(target, p):
        at = pl.ds(pl.multiple_of(target * HEAD_DIM, HEAD_DIM), HEAD_DIM)
        left = rows_all[:, :, :, at].reshape(total_rows, HEAD_DIM)
        right = kv_all[:, :, :, :, p * kv_width : (p + 1) * kv_width].reshape(total_rows, kv_width)
        return tn(left, right)

    depth = HEAD_DIM // SUBS

    def sum_copy(d, p, t, s):
        return remote(
            sbuf.at[d, p, t, s], rbuf.at[d, p, t, s], rs.at[d, p, t, s], rr.at[d, p, t, s], toward[d]
        )

    for t in range(long_way):
        for p in range(2):
            for d in range(2):
                if t >= hops[p][d]:
                    continue
                steps = hops[p][d] - t
                target = lax.rem(z + (steps if d == 0 else nz - steps), nz)
                mine = partial(target, p)
                for s in range(SUBS):
                    block = mine[s * depth : (s + 1) * depth, :]
                    if t > 0:
                        sum_copy(d, p, t - 1, s).wait_recv()
                        block = block + rbuf[d, p, t - 1, s].astype(F32)
                    sbuf[d, p, t, s] = block.astype(BF16)
                    push(sum_copy(d, p, t, s))
        if t == 0:
            own = lax.broadcasted_iota(jnp.int32, (16, nz * HEAD_DIM), 0) == xh * 2 + c
            totals = jnp.zeros((16, nz * HEAD_DIM), F32)
            for a in range(2):
                for b in range(2):
                    totals = totals + col_all[a, b].astype(F32)
            line = jnp.sum(jnp.where(own, totals, 0.0), axis=0, keepdims=True)
            for zz in range(nz):
                gsend[zz] = jnp.broadcast_to(line[:, head(zz)], (8, HEAD_DIM))
            for s in range(1, nz):
                push(
                    remote(
                        gsend.at[lax.rem(z + s, nz)], grecv.at[s - 1], gs.at[s - 1], gr.at[s - 1],
                        ring[s - 1],
                    )
                )
            for n in range(batches):
                first = plan_ref[n : n + 1, :] == 0
                for h in range(heads):
                    low_out[n, :, head(h)] = jnp.where(
                        first, low_s[0, :, head(h)].astype(F32), low_s[1, :, head(h)].astype(F32)
                    ).astype(BF16)
    outs = (key_out, value_out)
    for p in range(2):
        mine = partial(z, p)
        for s in range(SUBS):
            block = mine[s * depth : (s + 1) * depth, :]
            for d in range(2):
                last = hops[p][d] - 1
                sum_copy(d, p, last, s).wait_recv()
                block = block + rbuf[d, p, last, s].astype(F32)
            outs[p][s * depth : (s + 1) * depth, :] = block
    column = gsend[z]
    for s in range(1, nz):
        remote(gsend.at[0], grecv.at[s - 1], gs.at[s - 1], gr.at[s - 1], ring[s - 1]).wait_recv()
        column = column + grecv[s - 1]
    gain_out[...] = column

    for copy in sends:
        copy.wait_send()
    for n in range(3):
        row_copy(n).wait_send()
    for i in range(batches):
        for n in range(2):
            kv_copy(i, n).wait_send()

    @pl.when(section > 0)
    def _():
        for i in range(batches):
            for j in range(PIECES):
                outgoing(i, j).wait_send()

    @pl.when(section != sections - 2)
    def _():
        for i in range(batches):
            for n in range(len(DETOUR)):
                onward(i, n).wait_send()


def whole(x, cot, wk, wv, gain, plan, ny, nz):
    batches, tokens, width = x.shape
    depth, kv_width = wk.shape
    cosine, sine = rope_tables(tokens, HEAD_DIM)
    rows = batches * tokens
    half = nz // 2
    hop_ring = (2, 2, half, SUBS)
    dma = pltpu.SemaphoreType.DMA
    both = lambda *shape: [dma(shape), dma(shape)]
    via = len(DETOUR)
    return pl.pallas_call(
        functools.partial(kernel, ny, nz),
        out_shape=[
            jax.ShapeDtypeStruct((batches, tokens, width), BF16),
            jax.ShapeDtypeStruct((depth, kv_width), F32),
            jax.ShapeDtypeStruct((depth, kv_width), F32),
            jax.ShapeDtypeStruct((8, depth), F32),
        ],
        in_specs=[pl.BlockSpec(memory_space=pltpu.VMEM)] * 8,
        out_specs=[pl.BlockSpec(memory_space=pltpu.VMEM)] * 4,
        scratch_shapes=[
            pltpu.VMEM((2, nz, 2, depth, kv_width), BF16),
            pltpu.VMEM((2, nz, 2, depth, kv_width), BF16),
            pltpu.VMEM((2, nz, 2, 8, depth), F32),
            pltpu.VMEM((batches, tokens, width), BF16),
            pltpu.VMEM((batches, tokens, width), BF16),
            pltpu.VMEM((batches, via, tokens, width // PIECES), BF16),
            pltpu.VMEM((rows, width), BF16),
            pltpu.VMEM((2, 2, rows, nz * HEAD_DIM), BF16),
            pltpu.VMEM((2, 2, rows, nz * HEAD_DIM), BF16),
            pltpu.VMEM((batches, KV_HEADS, tokens, HEAD_DIM), BF16),
            pltpu.VMEM((batches, KV_HEADS, tokens, HEAD_DIM), BF16),
            pltpu.VMEM((batches, KV_HEADS, GROUP * tokens, HEAD_DIM), BF16),
            pltpu.VMEM((batches, KV_HEADS, tokens, GROUP * tokens), F32),
            pltpu.VMEM((rows, HEAD_DIM), F32),
            pltpu.VMEM((batches, tokens, width), F32),
            pltpu.VMEM((rows, kv_width), F32),
            pltpu.VMEM((rows, kv_width), F32),
            pltpu.VMEM((batches, tokens, 2 * kv_width), BF16),
            pltpu.VMEM((2, 2, batches, tokens, 2 * kv_width), BF16),
            pltpu.VMEM((16, nz * HEAD_DIM), BF16),
            pltpu.VMEM((2, 2, 16, nz * HEAD_DIM), BF16),
            pltpu.VMEM((*hop_ring, depth // SUBS, kv_width), BF16),
            pltpu.VMEM((*hop_ring, depth // SUBS, kv_width), BF16),
            pltpu.VMEM((nz, 8, HEAD_DIM), F32),
            pltpu.VMEM((nz - 1, 8, HEAD_DIM), F32),
            *both(3),
            *both(2, half, 2, 3),
            *both(1 + 2 * half),
            *both(3, 2, 1 + 2 * half),
            *both(batches, PIECES),
            *both(batches, via),
            dma((batches, via)),
            *both(3),
            *both(batches, 3),
            *both(3),
            *both(*hop_ring),
            *both(nz - 1),
        ],
        compiler_params=pltpu.CompilerParams(
            collective_id=0, has_side_effects=True, vmem_limit_bytes=VMEM_LIMIT
        ),
        name="whole",
    )(x, cot, wk, wv, gain, plan, jnp.asarray(cosine), jnp.asarray(sine))


def solution(mesh):
    sections, dp = mesh.shape["section"], mesh.shape["dp"]
    ny, nz = sections // 2, dp // 4
    split = Mesh(mesh.devices.reshape(ny, 2, 2, nz, 2), ("y", "xl", "xh", "z", "c"))

    def body(inputs, cotangent, norm_gain, key_weight, value_weight, plan):
        own_gain = jnp.broadcast_to(norm_gain[0].astype(F32)[None, :], (8, HEAD_DIM))
        order = jnp.broadcast_to(plan[0][:, None], (plan.shape[1], HEAD_DIM))
        low, key_grad, value_grad, gain_grad = whole(
            inputs[0], cotangent, key_weight[0], value_weight[0], own_gain, order, ny, nz
        )
        return low[None], key_grad[None], value_grad[None], gain_grad[0:1]

    placed = (
        P(SECTION, None, DP, None),
        P(None, DP, None),
        P(SECTION, DP),
        P(SECTION, DP, None),
        P(SECTION, DP, None),
        P(SECTION, None),
    )
    return jax.shard_map(
        body,
        mesh=split,
        in_specs=placed,
        out_specs=(
            P(SECTION, None, DP, None),
            P(SECTION, DP, None),
            P(SECTION, DP, None),
            P(SECTION, DP),
        ),
        check_vma=False,
    )
```

```python
import functools
import math

import jax
import jax.numpy as jnp
import numpy as np
from jax import lax
from jax.experimental import pallas as pl
from jax.experimental.pallas import tpu as pltpu
from jax.sharding import Mesh
from jax.sharding import PartitionSpec as P

MESH_ID = pl.DeviceIdType.MESH
KV_HEADS = 4
GROUP = 8
HEAD_DIM = 128
SECTION = ("y", "xl")
DP = ("xh", "z", "c")
eps = 1e-05
rope_base = 500000.0
VMEM_LIMIT = 60 * 1024 * 1024
F32 = jnp.float32
BF16 = jnp.bfloat16

PIECES = 8
DETOUR = (0, 1, 2, 3)
ALWAYS = (0, 1)
SEND_ORDER = (0, 4, 1, 5, 6, 2, 7, 3)
KEY_ORDER = (2, 3, 0, 1)
SUBS = 2


def rope_tables(length, head_dim):
    half = head_dim // 2
    exponent = -(np.arange(half, dtype=np.float32) * np.float32(2.0) / np.float32(head_dim))
    frequency = np.power(np.float32(rope_base), exponent).astype(np.float32)
    angles = np.arange(length, dtype=np.float32)[:, None] * frequency[None, :]
    cosine, sine = np.cos(angles), np.sin(angles)
    return (
        np.concatenate([cosine, cosine], axis=-1).astype(np.float32),
        np.concatenate([-sine, sine], axis=-1).astype(np.float32),
    )


def remote(src, dst, send, recv, peer):
    return pltpu.make_async_remote_copy(
        src_ref=src, dst_ref=dst, send_sem=send, recv_sem=recv, device_id=peer, device_id_type=MESH_ID
    )


def nn(a, b):
    return lax.dot_general(a, b, (((1,), (0,)), ((), ())), preferred_element_type=F32)


def nt(a, b):
    return lax.dot_general(a, b, (((1,), (1,)), ((), ())), preferred_element_type=F32)


def tn(a, b):
    return lax.dot_general(a, b, (((0,), (0,)), ((), ())), preferred_element_type=F32)


def head(h):
    return slice(h * HEAD_DIM, (h + 1) * HEAD_DIM)


def kernel(
    ny, nz,
    x_ref, cot_ref, wk_ref, wv_ref, gain_ref, plan_ref, cos_ref, sin_ref,
    low_out, key_out, value_out, gain_out,
    fk, fv, fg, gown, up_ref, low_s, via_ref, normed_s, out_rows, rows_all, key_s, value_s, query_s,
    prob_s, inv_s, qb_s, pre_k, pre_v, kv_s, kv_all, col_s, col_all, sbuf, rbuf, gsend, grecv,
    xs, xr, zs, zr, ws, wr, ds, dr, ls, lr, bs, br,
    us, ur, vs, vr, fs, ns, nr, ks, kr, cs, cr, rs, rr, gs, gr,
):
    y, xl = lax.axis_index("y"), lax.axis_index("xl")
    xh, z, c = lax.axis_index("xh"), lax.axis_index("z"), lax.axis_index("c")
    section, sections = y * 2 + xl, ny * 2
    batches, tokens, width = x_ref.shape
    kv_width = wk_ref.shape[1]
    heads = width // HEAD_DIM
    scale = 1.0 / math.sqrt(HEAD_DIM)

    def section_peer(steps):
        there = lax.rem(section + sections + steps, sections)
        return {"y": there // 2, "xl": lax.rem(there, 2)}

    below, above = section_peer(-1), section_peer(1)
    two_below, two_above = section_peer(-2), section_peer(2)
    across, partner, corner = {"xh": 1 - xh}, {"c": 1 - c}, {"xh": 1 - xh, "c": 1 - c}
    ring = [{"z": lax.rem(z + s, nz)} for s in range(1, nz)]
    toward = (ring[0], ring[nz - 2])
    long_way, short_way = nz // 2, nz - 1 - nz // 2

    gown[...] = jnp.broadcast_to(gain_ref[...].astype(F32), gown.shape)
    barrier = pltpu.get_barrier_semaphore()
    greeted = [across, partner, corner, below, above, two_below, two_above] + ring
    for peer in greeted:
        pl.semaphore_signal(barrier, inc=1, device_id=peer, device_id_type=MESH_ID)
    pl.semaphore_wait(barrier, len(greeted))

    sends = []

    def push(copy):
        copy.start()
        sends.append(copy)

    cosine, sine = cos_ref[...], sin_ref[...]

    def rotate(v):
        return v * cosine + pltpu.roll(v, HEAD_DIM // 2, axis=1) * sine

    def unrotate(v):
        return v * cosine - pltpu.roll(v, HEAD_DIM // 2, axis=1) * sine

    def gain(h):
        return fg[h // (2 * nz), h % 2, (h // 2) % nz, 0:1, :]

    sources, fulls = (wk_ref, wv_ref), (fk, fv)
    hops = ((long_way, short_way), (short_way, long_way))

    def place(p, src, steps, core=c):
        row = xh if src == 0 else 1 - xh
        return fulls[p].at[row, lax.rem(z + steps + nz, nz), core]

    def index_of(d, t):
        return 0 if t == 0 else 1 + long_way * d + t - 1

    def steps_of(d, t):
        return -t if d == 0 else t

    def share(p, src, data, slot, index):
        push(remote(data, slot, ds.at[p, src, index], dr.at[p, src, index], partner))

    def ring_copy(data, slot, d, t, src, p):
        return remote(data, slot, zs.at[d, t, src, p], zr.at[d, t, src, p], toward[d])

    def first_moves(p):
        slot = place(p, 0, 0)
        for d in range(2):
            push(ring_copy(sources[p], slot, d, 0, 0, p))
        share(p, 0, sources[p], slot, 0)
        fulls[p][xh, z, c] = sources[p][...]

    def gain_block(row, core, n, peer):
        slot = fg.at[row, core]
        return remote(slot, slot, bs.at[n], br.at[n], peer)

    def row_arrival(p):
        slot = place(p, 1, 0)
        remote(slot, slot, xs.at[p], xr.at[p], across).wait_recv()
        for d in range(2):
            push(ring_copy(slot, slot, d, 0, 1, p))
        share(p, 1, slot, slot, 0)

    def ring_arrival(p, src, d, t):
        if t > hops[p][d]:
            return
        slot = place(p, src, steps_of(d, t))
        ring_copy(slot, slot, d, t - 1, src, p).wait_recv()
        if t < hops[p][d]:
            push(ring_copy(slot, slot, d, t, src, p))
        index = index_of(d, t)
        if p == 1:
            push(remote(slot, slot, ws.at[index], wr.at[index], across))
        share(p, src, slot, slot, index)

    def cross_arrival(d, t):
        if t > hops[1][d]:
            return
        index = index_of(d, t)
        slot = place(1, 1, steps_of(d, t))
        remote(slot, slot, ws.at[index], wr.at[index], across).wait_recv()
        share(1, 1, slot, slot, index)

    def shared_arrivals(p):
        for src in range(2):
            for d in range(2):
                for t in range(hops[p][d] + 1):
                    if t == 0 and d == 1:
                        continue
                    index = index_of(d, t)
                    slot = place(p, src, steps_of(d, t), 1 - c)
                    remote(slot, slot, ds.at[p, src, index], dr.at[p, src, index], partner).wait_recv()

    def mean_square(i):
        here = slice(i * tokens, (i + 1) * tokens)
        total = jnp.zeros((tokens, HEAD_DIM), F32)
        for h in range(heads):
            piece = x_ref[i, :, head(h)].astype(F32)
            total = total + piece * piece
        inv = lax.rsqrt(jnp.sum(total, axis=-1, keepdims=True) * (1.0 / width) + eps)
        inv_s[here, :] = jnp.broadcast_to(inv, (tokens, HEAD_DIM))

    def normalise(i, h):
        here = slice(i * tokens, (i + 1) * tokens)
        piece = x_ref[i, :, head(h)].astype(F32)
        normed = (piece * inv_s[here, :] * gain(h)).astype(BF16)
        normed_s[here, head(h)] = normed
        out_rows[h // (2 * nz), h % 2, here, head((h // 2) % nz)] = normed
        rows = slice((h % GROUP) * tokens, (h % GROUP + 1) * tokens)
        query_s[i, h // GROUP, rows, :] = rotate(normed.astype(F32)).astype(BF16)

    for n in range(1, nz):
        push(remote(gown, fg.at[xh, c, z], ls.at[n - 1], lr.at[n - 1], ring[n - 1]))
    first_moves(0)
    first_moves(1)
    fg[xh, c, z] = gown[...]
    mean_square(0)
    mean_square(1)
    for n in range(1, nz):
        slot = fg.at[xh, c, lax.rem(z + nz - n, nz)]
        remote(slot, slot, ls.at[n - 1], lr.at[n - 1], ring[n - 1]).wait_recv()
    for n, peer in enumerate((partner, across)):
        push(gain_block(xh, c, n, peer))
    push(remote(sources[0], place(0, 0, 0), xs.at[0], xr.at[0], across))
    push(remote(sources[1], place(1, 0, 0), ws.at[0], wr.at[0], across))
    waiting = [(i, h) for i in range(batches) for h in range(heads)]
    share_of = -(-len(waiting) // (2 * long_way - 2))

    def some_work():
        for _ in range(min(share_of, len(waiting))):
            normalise(*waiting.pop(0))

    for t in range(1, long_way + 1):
        for d in range(2):
            ring_arrival(0, 0, d, t)
            ring_arrival(1, 0, d, t)
        if t == 1:
            row_arrival(0)
            gain_block(1 - xh, c, 1, across).wait_recv()
            push(gain_block(1 - xh, c, 2, partner))
        else:
            some_work()
        for d in range(2):
            ring_arrival(0, 1, d, t)
            if t > 1 or d == 0:
                cross_arrival(d, t - 1)
        if t == 1:
            gain_block(xh, 1 - c, 0, partner).wait_recv()
            gain_block(1 - xh, 1 - c, 2, partner).wait_recv()
        else:
            some_work()
    while waiting:
        some_work()
    for d in range(2):
        cross_arrival(d, long_way)
    shared_arrivals(0)
    shared_arrivals(1)
    wk, wv = fk.reshape(width, kv_width), fv.reshape(width, kv_width)

    near = ((xh, 1 - c), (1 - xh, c), (1 - xh, 1 - c))
    row_peers = (partner, across, corner)

    def row_copy(n):
        return remote(
            out_rows.at[near[n][0], near[n][1]], rows_all.at[xh, c], ns.at[n], nr.at[n], row_peers[n]
        )

    rows_all[xh, c] = out_rows[xh, c]

    @pl.when(section < sections - 2)
    def _():
        for n in range(3):
            row_copy(n).start()

    key_pre = nn(normed_s[...], wk[...])
    value_pre = nn(normed_s[...], wv[...])
    pre_k[...] = key_pre
    pre_v[...] = value_pre
    m_at = lax.broadcasted_iota(jnp.int32, (tokens, GROUP * tokens), 0)
    l_at = lax.rem(lax.broadcasted_iota(jnp.int32, (tokens, GROUP * tokens), 1), tokens)
    causal = m_at <= l_at
    for i in range(batches):
        here = slice(i * tokens, (i + 1) * tokens)
        for k in range(KV_HEADS):
            key_s[i, k] = rotate(key_pre[here, head(k)]).astype(BF16)
            value_s[i, k] = value_pre[here, head(k)].astype(BF16)
            scores = nt(key_s[i, k], query_s[i, k]) * scale
            raised = jnp.where(causal, jnp.exp(scores), 0.0)
            prob_s[i, k] = raised / jnp.sum(raised, axis=0, keepdims=True)

    piece_width = width // PIECES
    piece_heads = heads // PIECES

    @pl.when(section == sections - 1)
    def _():
        up_ref[...] = cot_ref[...]

    def piece(ref, i, j):
        return ref.at[i, :, pl.ds(j * piece_width, piece_width)]

    def direct(i, j):
        return remote(piece(low_s, i, j), piece(up_ref, i, j), us.at[i, j], ur.at[i, j], below)

    def roundabout(i, j):
        n = DETOUR.index(j)
        return remote(piece(low_s, i, j), via_ref.at[i, n], us.at[i, j], vr.at[i, n], two_below)

    def send_piece(i, j):
        if j in DETOUR:

            @pl.when((section > 0) if j in ALWAYS else (section > 0) & (xl == 0))
            def _():
                roundabout(i, j).start()

        if j not in ALWAYS:

            @pl.when((xl == 1) if j in DETOUR else section > 0)
            def _():
                direct(i, j).start()

    def onward(i, n):
        return remote(
            via_ref.at[i, n], piece(up_ref, i, DETOUR[n]), fs.at[i, n], ur.at[i, DETOUR[n]], above
        )

    def pass_on(i):
        def one(n):
            remote(via_ref.at[i, n], via_ref.at[i, n], fs.at[i, n], vr.at[i, n], above).wait_recv()
            onward(i, n).start()

        for n, j in enumerate(DETOUR):
            if j in ALWAYS:
                one(n)
            else:
                pl.when(xl == 0)(functools.partial(one, n))

    def kv_copy(i, n):
        peer = (partner, across)[n]
        return remote(kv_s.at[i], kv_all.at[xh, c, i], ks.at[i, n], kr.at[i, n], peer)

    @pl.when(section < sections - 2)
    def _():
        for i in range(batches):
            pass_on(i)

    def one_batch(i, carry):
        start = pl.multiple_of(i * tokens, tokens)
        here = pl.ds(start, tokens)
        inv = inv_s[here, :]
        mean = jnp.zeros((tokens, HEAD_DIM), F32)
        for k in KEY_ORDER:

            @pl.when(section < sections - 1)
            def _():
                for j in (2 * k, 2 * k + 1):
                    slot = piece(up_ref, i, j)
                    remote(slot, slot, us.at[i, j], ur.at[i, j], below).wait_recv()

            upper = jnp.concatenate(
                [up_ref[i, :, head(k * GROUP + h)] for h in range(GROUP)], axis=0
            )
            prob = prob_s[i, k]
            grad_prob = nt(value_s[i, k], upper)
            grad_value = nn(prob.astype(BF16), upper).astype(BF16)
            row_dot = jnp.sum(prob * grad_prob, axis=0, keepdims=True)
            grad_score = (prob * (grad_prob - row_dot) * scale).astype(BF16)
            grad_query = tn(grad_score, key_s[i, k])
            key_back = unrotate(nn(grad_score, query_s[i, k])).astype(BF16)
            kv_s[i, :, head(k)] = key_back
            kv_s[i, :, head(KV_HEADS + k)] = grad_value
            mean = mean + key_back.astype(F32) * pre_k[here, head(k)]
            mean = mean + grad_value.astype(F32) * pre_v[here, head(k)]
            for h in range(GROUP):
                at = head(k * GROUP + h)
                query_back = unrotate(grad_query[h * tokens : (h + 1) * tokens, :])
                qb_s[i, :, at] = query_back
                mean = mean + query_back * (
                    x_ref[i, :, at].astype(F32) * inv * gain(k * GROUP + h)
                )
        row_mean = jnp.sum(mean, axis=-1, keepdims=True) * (1.0 / width)
        drop = inv * inv * row_mean
        key_flat = kv_s[i, :, 0:kv_width]
        value_flat = kv_s[i, :, kv_width : 2 * kv_width]
        for j in SEND_ORDER:
            cols = slice(j * piece_width, (j + 1) * piece_width)
            projected = nt(key_flat, wk[cols, :]) + nt(value_flat, wv[cols, :])
            for h in range(piece_heads):
                at = head(j * piece_heads + h)
                grad_normed = qb_s[i, :, at] + projected[:, head(h)]
                qb_s[i, :, at] = grad_normed
                low_s[i, :, at] = (
                    up_ref[i, :, at].astype(F32)
                    + inv * gain(j * piece_heads + h) * grad_normed
                    - x_ref[i, :, at].astype(F32) * drop
                ).astype(BF16)

            send_piece(i, j)

        @pl.when(section == 0)
        def _():
            for n in range(2):
                kv_copy(i, n).start()

        return carry

    lax.fori_loop(0, batches, one_batch, 0)

    @pl.when(section > 0)
    def _():
        for i in range(batches):
            for n in range(2):
                kv_copy(i, n).start()

    @pl.when(section >= sections - 2)
    def _():
        for n in range(3):
            row_copy(n).start()

    @pl.when(section == sections - 1)
    def _():
        for i in range(batches):
            pass_on(i)

    columns = []
    for h in range(heads):
        at = head(h)
        total = jnp.zeros((8, HEAD_DIM), F32)
        for i in range(batches):
            here = slice(i * tokens, (i + 1) * tokens)
            term = qb_s[i, :, at] * x_ref[i, :, at].astype(F32) * inv_s[here, :]
            total = total + jnp.sum(term.reshape(tokens // 8, 8, HEAD_DIM), axis=0)
        columns.append(jnp.sum(total, axis=0, keepdims=True))
    lines = [
        jnp.concatenate([columns[a * 2 * nz + 2 * zz + b] for zz in range(nz)], axis=1)
        for a in range(2)
        for b in range(2)
    ]
    lines.append(jnp.zeros((12, nz * HEAD_DIM), F32))
    col_s[...] = jnp.concatenate(lines, axis=0).astype(BF16)
    kv_all[xh, c] = kv_s[...]
    col_all[xh, c] = col_s[...]
    for n, peer in enumerate((partner, across)):
        push(remote(col_s, col_all.at[xh, c], cs.at[n], cr.at[n], peer))
    for i in range(batches):
        slot = kv_all.at[1 - xh, c, i]
        remote(slot, slot, ks.at[i, 1], kr.at[i, 1], across).wait_recv()
        push(remote(slot, slot, ks.at[i, 2], kr.at[i, 2], partner))
    slot = col_all.at[1 - xh, c]
    remote(slot, slot, cs.at[1], cr.at[1], across).wait_recv()
    push(remote(slot, slot, cs.at[2], cr.at[2], partner))
    for n in range(3):
        slot = rows_all.at[near[n][0], near[n][1]]
        remote(slot, slot, ns.at[n], nr.at[n], row_peers[n]).wait_recv()
    for n, a in ((0, xh), (2, 1 - xh)):
        for i in range(batches):
            slot = kv_all.at[a, 1 - c, i]
            remote(slot, slot, ks.at[i, n], kr.at[i, n], partner).wait_recv()
        slot = col_all.at[a, 1 - c]
        remote(slot, slot, cs.at[n], cr.at[n], partner).wait_recv()

    total_rows = 4 * batches * tokens

    def partial(target, p):
        at = pl.ds(pl.multiple_of(target * HEAD_DIM, HEAD_DIM), HEAD_DIM)
        left = rows_all[:, :, :, at].reshape(total_rows, HEAD_DIM)
        right = kv_all[:, :, :, :, p * kv_width : (p + 1) * kv_width].reshape(total_rows, kv_width)
        return tn(left, right)

    depth = HEAD_DIM // SUBS

    def sum_copy(d, p, t, s):
        return remote(
            sbuf.at[d, p, t, s], rbuf.at[d, p, t, s], rs.at[d, p, t, s], rr.at[d, p, t, s], toward[d]
        )

    for t in range(long_way):
        for p in range(2):
            for d in range(2):
                if t >= hops[p][d]:
                    continue
                steps = hops[p][d] - t
                target = lax.rem(z + (steps if d == 0 else nz - steps), nz)
                mine = partial(target, p)
                for s in range(SUBS):
                    block = mine[s * depth : (s + 1) * depth, :]
                    if t > 0:
                        sum_copy(d, p, t - 1, s).wait_recv()
                        block = block + rbuf[d, p, t - 1, s].astype(F32)
                    sbuf[d, p, t, s] = block.astype(BF16)
                    push(sum_copy(d, p, t, s))
        if t == 0:
            own = lax.broadcasted_iota(jnp.int32, (16, nz * HEAD_DIM), 0) == xh * 2 + c
            totals = jnp.zeros((16, nz * HEAD_DIM), F32)
            for a in range(2):
                for b in range(2):
                    totals = totals + col_all[a, b].astype(F32)
            line = jnp.sum(jnp.where(own, totals, 0.0), axis=0, keepdims=True)
            for zz in range(nz):
                gsend[zz] = jnp.broadcast_to(line[:, head(zz)], (8, HEAD_DIM))
            for s in range(1, nz):
                push(
                    remote(
                        gsend.at[lax.rem(z + s, nz)], grecv.at[s - 1], gs.at[s - 1], gr.at[s - 1],
                        ring[s - 1],
                    )
                )
            for n in range(batches):
                first = plan_ref[0, n] == 0
                for h in range(heads):
                    low_out[n, :, head(h)] = jnp.where(
                        first, low_s[0, :, head(h)].astype(F32), low_s[1, :, head(h)].astype(F32)
                    ).astype(BF16)
    outs = (key_out, value_out)
    for p in range(2):
        mine = partial(z, p)
        for s in range(SUBS):
            block = mine[s * depth : (s + 1) * depth, :]
            for d in range(2):
                last = hops[p][d] - 1
                sum_copy(d, p, last, s).wait_recv()
                block = block + rbuf[d, p, last, s].astype(F32)
            outs[p][s * depth : (s + 1) * depth, :] = block
    column = gsend[z]
    for s in range(1, nz):
        remote(gsend.at[0], grecv.at[s - 1], gs.at[s - 1], gr.at[s - 1], ring[s - 1]).wait_recv()
        column = column + grecv[s - 1]
    gain_out[...] = column[0:1, :]

    for copy in sends:
        copy.wait_send()
    for n in range(3):
        row_copy(n).wait_send()
    for i in range(batches):
        for n in range(2):
            kv_copy(i, n).wait_send()

    @pl.when(section > 0)
    def _():
        for i in range(batches):
            for j in range(PIECES):
                direct(i, j).wait_send()

    @pl.when(section != sections - 2)
    def _():
        for i in range(batches):
            for n in range(len(ALWAYS)):
                onward(i, n).wait_send()

    @pl.when((section < sections - 2) & (xl == 0))
    def _():
        for i in range(batches):
            for n in range(len(ALWAYS), len(DETOUR)):
                onward(i, n).wait_send()


def whole(x, cot, wk, wv, gain, plan, ny, nz):
    batches, tokens, width = x.shape
    depth, kv_width = wk.shape
    cosine, sine = rope_tables(tokens, HEAD_DIM)
    rows = batches * tokens
    half = nz // 2
    hop_ring = (2, 2, half, SUBS)
    dma = pltpu.SemaphoreType.DMA
    both = lambda *shape: [dma(shape), dma(shape)]
    via = len(DETOUR)
    return pl.pallas_call(
        functools.partial(kernel, ny, nz),
        out_shape=[
            jax.ShapeDtypeStruct((batches, tokens, width), BF16),
            jax.ShapeDtypeStruct((depth, kv_width), F32),
            jax.ShapeDtypeStruct((depth, kv_width), F32),
            jax.ShapeDtypeStruct((1, depth), F32),
        ],
        in_specs=[pl.BlockSpec(memory_space=pltpu.VMEM)] * 5
        + [pl.BlockSpec(memory_space=pltpu.SMEM)]
        + [pl.BlockSpec(memory_space=pltpu.VMEM)] * 2,
        out_specs=[pl.BlockSpec(memory_space=pltpu.VMEM)] * 4,
        scratch_shapes=[
            pltpu.VMEM((2, nz, 2, depth, kv_width), BF16),
            pltpu.VMEM((2, nz, 2, depth, kv_width), BF16),
            pltpu.VMEM((2, 2, nz, 8, depth), F32),
            pltpu.VMEM((8, depth), F32),
            pltpu.VMEM((batches, tokens, width), BF16),
            pltpu.VMEM((batches, tokens, width), BF16),
            pltpu.VMEM((batches, via, tokens, width // PIECES), BF16),
            pltpu.VMEM((rows, width), BF16),
            pltpu.VMEM((2, 2, rows, nz * HEAD_DIM), BF16),
            pltpu.VMEM((2, 2, rows, nz * HEAD_DIM), BF16),
            pltpu.VMEM((batches, KV_HEADS, tokens, HEAD_DIM), BF16),
            pltpu.VMEM((batches, KV_HEADS, tokens, HEAD_DIM), BF16),
            pltpu.VMEM((batches, KV_HEADS, GROUP * tokens, HEAD_DIM), BF16),
            pltpu.VMEM((batches, KV_HEADS, tokens, GROUP * tokens), F32),
            pltpu.VMEM((rows, HEAD_DIM), F32),
            pltpu.VMEM((batches, tokens, width), F32),
            pltpu.VMEM((rows, kv_width), F32),
            pltpu.VMEM((rows, kv_width), F32),
            pltpu.VMEM((batches, tokens, 2 * kv_width), BF16),
            pltpu.VMEM((2, 2, batches, tokens, 2 * kv_width), BF16),
            pltpu.VMEM((16, nz * HEAD_DIM), BF16),
            pltpu.VMEM((2, 2, 16, nz * HEAD_DIM), BF16),
            pltpu.VMEM((*hop_ring, depth // SUBS, kv_width), BF16),
            pltpu.VMEM((*hop_ring, depth // SUBS, kv_width), BF16),
            pltpu.VMEM((nz, 8, HEAD_DIM), F32),
            pltpu.VMEM((nz - 1, 8, HEAD_DIM), F32),
            *both(1),
            *both(2, half, 2, 2),
            *both(1 + 2 * half),
            *both(2, 2, 1 + 2 * half),
            *both(nz - 1),
            *both(3),
            *both(batches, PIECES),
            *both(batches, via),
            dma((batches, via)),
            *both(3),
            *both(batches, 3),
            *both(3),
            *both(*hop_ring),
            *both(nz - 1),
        ],
        compiler_params=pltpu.CompilerParams(
            collective_id=0, has_side_effects=True, vmem_limit_bytes=VMEM_LIMIT
        ),
        name="whole",
    )(x, cot, wk, wv, gain, plan, jnp.asarray(cosine), jnp.asarray(sine))


def solution(mesh):
    sections, dp = mesh.shape["section"], mesh.shape["dp"]
    ny, nz = sections // 2, dp // 4
    split = Mesh(mesh.devices.reshape(ny, 2, 2, nz, 2), ("y", "xl", "xh", "z", "c"))

    def body(inputs, cotangent, norm_gain, key_weight, value_weight, plan):
        low, key_grad, value_grad, gain_grad = whole(
            inputs[0], cotangent, key_weight[0], value_weight[0], norm_gain, plan, ny, nz
        )
        return low[None], key_grad[None], value_grad[None], gain_grad

    placed = (
        P(SECTION, None, DP, None),
        P(None, DP, None),
        P(SECTION, DP),
        P(SECTION, DP, None),
        P(SECTION, DP, None),
        P(SECTION, None),
    )
    return jax.shard_map(
        body,
        mesh=split,
        in_specs=placed,
        out_specs=(
            P(SECTION, None, DP, None),
            P(SECTION, DP, None),
            P(SECTION, DP, None),
            P(SECTION, DP),
        ),
        check_vma=False,
    )
```

```python
import functools
import math

import jax
import jax.numpy as jnp
import numpy as np
from jax import lax
from jax.experimental import pallas as pl
from jax.experimental.pallas import tpu as pltpu
from jax.sharding import Mesh
from jax.sharding import PartitionSpec as P

MESH_ID = pl.DeviceIdType.MESH
KV_HEADS = 4
GROUP = 8
HEAD_DIM = 128
SECTION = ("y", "xl")
DP = ("xh", "z", "c")
eps = 1e-05
rope_base = 500000.0
VMEM_LIMIT = 60 * 1024 * 1024
F32 = jnp.float32
BF16 = jnp.bfloat16

PIECES = 8
EVEN_DOWN = (0, 1, 2, 3)
ODD_DOWN = (0,)
ODD_UP = (2, 3)
DOWN = tuple(sorted(set(EVEN_DOWN + ODD_DOWN)))
SEND_ORDER = (0, 4, 1, 5, 2, 6, 3, 7)
KEY_ORDER = (2, 3, 0, 1)
SUBS = 2


def rope_tables(length, head_dim):
    half = head_dim // 2
    exponent = -(np.arange(half, dtype=np.float32) * np.float32(2.0) / np.float32(head_dim))
    frequency = np.power(np.float32(rope_base), exponent).astype(np.float32)
    angles = np.arange(length, dtype=np.float32)[:, None] * frequency[None, :]
    cosine, sine = np.cos(angles), np.sin(angles)
    return (
        np.concatenate([cosine, cosine], axis=-1).astype(np.float32),
        np.concatenate([-sine, sine], axis=-1).astype(np.float32),
    )


def remote(src, dst, send, recv, peer):
    return pltpu.make_async_remote_copy(
        src_ref=src, dst_ref=dst, send_sem=send, recv_sem=recv, device_id=peer, device_id_type=MESH_ID
    )


def nn(a, b):
    return lax.dot_general(a, b, (((1,), (0,)), ((), ())), preferred_element_type=F32)


def nt(a, b):
    return lax.dot_general(a, b, (((1,), (1,)), ((), ())), preferred_element_type=F32)


def tn(a, b):
    return lax.dot_general(a, b, (((0,), (0,)), ((), ())), preferred_element_type=F32)


def head(h):
    return slice(h * HEAD_DIM, (h + 1) * HEAD_DIM)


def kernel(
    ny, nz,
    x_ref, cot_ref, wk_ref, wv_ref, gain_ref, plan_ref, cos_ref, sin_ref,
    low_out, key_out, value_out, gain_out,
    fk, fv, fg, gown, up_ref, low_s, via_ref, hill_ref, normed_s, out_rows, rows_all, key_s, value_s, query_s,
    prob_s, inv_s, drop_s, qb_s, pre_k, pre_v, kv_s, kv_all, col_s, col_all, sbuf, rbuf, gsend, grecv,
    xs, xr, zs, zr, ws, wr, ds, dr, ls, lr, bs, br,
    us, ur, vs, vr, fs, hs, hr, ns, nr, ks, kr, cs, cr, rs, rr, gs, gr,
):
    y, xl = lax.axis_index("y"), lax.axis_index("xl")
    xh, z, c = lax.axis_index("xh"), lax.axis_index("z"), lax.axis_index("c")
    section, sections = y * 2 + xl, ny * 2
    batches, tokens, width = x_ref.shape
    kv_width = wk_ref.shape[1]
    heads = width // HEAD_DIM
    scale = 1.0 / math.sqrt(HEAD_DIM)

    def section_peer(steps):
        there = lax.rem(section + sections + steps, sections)
        return {"y": there // 2, "xl": lax.rem(there, 2)}

    below, above = section_peer(-1), section_peer(1)
    two_below, two_above = section_peer(-2), section_peer(2)
    three_below, three_above = section_peer(-3), section_peer(3)
    across, partner, corner = {"xh": 1 - xh}, {"c": 1 - c}, {"xh": 1 - xh, "c": 1 - c}
    ring = [{"z": lax.rem(z + s, nz)} for s in range(1, nz)]
    toward = (ring[0], ring[nz - 2])
    long_way, short_way = nz // 2, nz - 1 - nz // 2

    gown[...] = jnp.broadcast_to(gain_ref[...].astype(F32), gown.shape)
    barrier = pltpu.get_barrier_semaphore()
    greeted = [across, partner, corner, below, above, two_below, two_above]
    greeted += [three_below, three_above] + ring
    for peer in greeted:
        pl.semaphore_signal(barrier, inc=1, device_id=peer, device_id_type=MESH_ID)
    pl.semaphore_wait(barrier, len(greeted))

    sends = []

    def push(copy):
        copy.start()
        sends.append(copy)

    cosine, sine = cos_ref[...], sin_ref[...]

    def rotate(v):
        return v * cosine + pltpu.roll(v, HEAD_DIM // 2, axis=1) * sine

    def unrotate(v):
        return v * cosine - pltpu.roll(v, HEAD_DIM // 2, axis=1) * sine

    def gain(h):
        return fg[h // (2 * nz), h % 2, (h // 2) % nz, 0:1, :]

    sources, fulls = (wk_ref, wv_ref), (fk, fv)
    hops = ((long_way, short_way), (short_way, long_way))

    def place(p, src, steps, core=c):
        row = xh if src == 0 else 1 - xh
        return fulls[p].at[row, lax.rem(z + steps + nz, nz), core]

    def index_of(d, t):
        return 0 if t == 0 else 1 + long_way * d + t - 1

    def steps_of(d, t):
        return -t if d == 0 else t

    def share(p, src, data, slot, index):
        push(remote(data, slot, ds.at[p, src, index], dr.at[p, src, index], partner))

    def ring_copy(data, slot, d, t, src, p):
        return remote(data, slot, zs.at[d, t, src, p], zr.at[d, t, src, p], toward[d])

    def first_moves(p):
        slot = place(p, 0, 0)
        for d in range(2):
            push(ring_copy(sources[p], slot, d, 0, 0, p))
        share(p, 0, sources[p], slot, 0)
        fulls[p][xh, z, c] = sources[p][...]

    def gain_block(row, core, n, peer):
        slot = fg.at[row, core]
        return remote(slot, slot, bs.at[n], br.at[n], peer)

    def row_arrival(p):
        slot = place(p, 1, 0)
        remote(slot, slot, xs.at[p], xr.at[p], across).wait_recv()
        for d in range(2):
            push(ring_copy(slot, slot, d, 0, 1, p))
        share(p, 1, slot, slot, 0)

    def ring_arrival(p, src, d, t):
        if t > hops[p][d]:
            return
        slot = place(p, src, steps_of(d, t))
        ring_copy(slot, slot, d, t - 1, src, p).wait_recv()
        if t < hops[p][d]:
            push(ring_copy(slot, slot, d, t, src, p))
        index = index_of(d, t)
        if p == 1:
            push(remote(slot, slot, ws.at[index], wr.at[index], across))
        share(p, src, slot, slot, index)

    def cross_arrival(d, t):
        if t > hops[1][d]:
            return
        index = index_of(d, t)
        slot = place(1, 1, steps_of(d, t))
        remote(slot, slot, ws.at[index], wr.at[index], across).wait_recv()
        share(1, 1, slot, slot, index)

    def shared_arrivals(p):
        for src in range(2):
            for d in range(2):
                for t in range(hops[p][d] + 1):
                    if t == 0 and d == 1:
                        continue
                    index = index_of(d, t)
                    slot = place(p, src, steps_of(d, t), 1 - c)
                    remote(slot, slot, ds.at[p, src, index], dr.at[p, src, index], partner).wait_recv()

    def mean_square(i):
        here = slice(i * tokens, (i + 1) * tokens)
        total = jnp.zeros((tokens, HEAD_DIM), F32)
        for h in range(heads):
            piece = x_ref[i, :, head(h)].astype(F32)
            total = total + piece * piece
        inv = lax.rsqrt(jnp.sum(total, axis=-1, keepdims=True) * (1.0 / width) + eps)
        inv_s[here, :] = jnp.broadcast_to(inv, (tokens, HEAD_DIM))

    def normalise(i, h):
        here = slice(i * tokens, (i + 1) * tokens)
        piece = x_ref[i, :, head(h)].astype(F32)
        normed = (piece * inv_s[here, :] * gain(h)).astype(BF16)
        normed_s[here, head(h)] = normed
        out_rows[h // (2 * nz), h % 2, here, head((h // 2) % nz)] = normed
        rows = slice((h % GROUP) * tokens, (h % GROUP + 1) * tokens)
        query_s[i, h // GROUP, rows, :] = rotate(normed.astype(F32)).astype(BF16)

    for n in range(1, nz):
        push(remote(gown, fg.at[xh, c, z], ls.at[n - 1], lr.at[n - 1], ring[n - 1]))
    first_moves(0)
    first_moves(1)
    fg[xh, c, z] = gown[...]
    push(remote(sources[0], place(0, 0, 0), xs.at[0], xr.at[0], across))
    push(remote(sources[1], place(1, 0, 0), ws.at[0], wr.at[0], across))
    mean_square(0)
    mean_square(1)

    def own_gains():
        for n in range(1, nz):
            slot = fg.at[xh, c, lax.rem(z + nz - n, nz)]
            remote(slot, slot, ls.at[n - 1], lr.at[n - 1], ring[n - 1]).wait_recv()
        for n, peer in enumerate((partner, across)):
            push(gain_block(xh, c, n, peer))

    waiting = [(i, h) for i in range(batches) for h in range(heads)]
    share_of = -(-len(waiting) // (2 * long_way - 4))

    def some_work():
        for _ in range(min(share_of, len(waiting))):
            normalise(*waiting.pop(0))

    for t in range(1, long_way + 1):
        for d in range(2):
            ring_arrival(0, 0, d, t)
            ring_arrival(1, 0, d, t)
        if t == 1:
            row_arrival(0)
            own_gains()
        elif t == 2:
            gain_block(1 - xh, c, 1, across).wait_recv()
            push(gain_block(1 - xh, c, 2, partner))
        else:
            some_work()
        for d in range(2):
            ring_arrival(0, 1, d, t)
            if t > 1 or d == 0:
                cross_arrival(d, t - 1)
        if t == 2:
            gain_block(xh, 1 - c, 0, partner).wait_recv()
            gain_block(1 - xh, 1 - c, 2, partner).wait_recv()
        elif t > 2:
            some_work()
    while waiting:
        some_work()
    for d in range(2):
        cross_arrival(d, long_way)
    shared_arrivals(0)
    shared_arrivals(1)
    wk, wv = fk.reshape(width, kv_width), fv.reshape(width, kv_width)

    near = ((xh, 1 - c), (1 - xh, c), (1 - xh, 1 - c))
    row_peers = (partner, across, corner)

    def row_copy(n):
        return remote(
            out_rows.at[near[n][0], near[n][1]], rows_all.at[xh, c], ns.at[n], nr.at[n], row_peers[n]
        )

    rows_all[xh, c] = out_rows[xh, c]

    @pl.when(section < sections - 2)
    def _():
        for n in range(3):
            row_copy(n).start()

    pre_k[...] = nn(normed_s[...], wk[...])
    pre_v[...] = nn(normed_s[...], wv[...])
    m_at = lax.broadcasted_iota(jnp.int32, (tokens, GROUP * tokens), 0)
    l_at = lax.rem(lax.broadcasted_iota(jnp.int32, (tokens, GROUP * tokens), 1), tokens)
    causal = m_at <= l_at

    def attend(i):
        here = slice(i * tokens, (i + 1) * tokens)
        for k in range(KV_HEADS):
            key_s[i, k] = rotate(pre_k[here, head(k)]).astype(BF16)
            value_s[i, k] = pre_v[here, head(k)].astype(BF16)
            scores = nt(key_s[i, k], query_s[i, k]) * scale
            raised = jnp.where(causal, jnp.exp(scores), 0.0)
            prob_s[i, k] = raised / jnp.sum(raised, axis=0, keepdims=True)

    attend(0)

    @pl.when(section < sections - 1)
    def _():
        attend(1)

    piece_width = width // PIECES
    piece_heads = heads // PIECES

    @pl.when(section == sections - 1)
    def _():
        up_ref[...] = cot_ref[...]

    def piece(ref, i, j):
        return ref.at[i, :, pl.ds(j * piece_width, piece_width)]

    def direct(i, j):
        return remote(piece(low_s, i, j), piece(up_ref, i, j), us.at[i, j], ur.at[i, j], below)

    def roundabout(i, j):
        n = DOWN.index(j)
        return remote(piece(low_s, i, j), via_ref.at[i, n], us.at[i, j], vr.at[i, n], two_below)

    def uphill(i, j):
        n = ODD_UP.index(j)
        return remote(piece(low_s, i, j), hill_ref.at[i, n], us.at[i, j], hr.at[i, n], two_above)

    def over(i, n):
        j = ODD_UP[n]
        return remote(hill_ref.at[i, n], piece(up_ref, i, j), hs.at[i, n], ur.at[i, j], three_below)

    def hand_down(i):
        for n in range(len(ODD_UP)):
            slot = hill_ref.at[i, n]
            remote(slot, slot, hs.at[i, n], hr.at[i, n], three_below).wait_recv()
            over(i, n).start()

    def on_parity(even, odd, run, base=None):
        if even and odd:
            run() if base is None else pl.when(base)(run)
        elif even:
            pl.when((xl == 0) if base is None else (xl == 0) & base)(run)
        elif odd:
            pl.when((xl == 1) if base is None else (xl == 1) & base)(run)

    def send_piece(i, j):
        on_parity(j in EVEN_DOWN, j in ODD_DOWN, lambda: roundabout(i, j).start(), section > 0)
        on_parity(False, j in ODD_UP, lambda: uphill(i, j).start())
        on_parity(
            j not in EVEN_DOWN, j not in ODD_DOWN + ODD_UP, lambda: direct(i, j).start(), section > 0
        )

    def onward(i, n):
        return remote(
            via_ref.at[i, n], piece(up_ref, i, DOWN[n]), fs.at[i, n], ur.at[i, DOWN[n]], above
        )

    def pass_piece(i, n):
        remote(via_ref.at[i, n], via_ref.at[i, n], fs.at[i, n], vr.at[i, n], above).wait_recv()
        onward(i, n).start()

    def pass_on(i):
        for n, j in enumerate(DOWN):
            on_parity(j in EVEN_DOWN, j in ODD_DOWN, functools.partial(pass_piece, i, n))

    def kv_copy(i, n):
        peer = (partner, across)[n]
        return remote(kv_s.at[i], kv_all.at[xh, c, i], ks.at[i, n], kr.at[i, n], peer)

    @pl.when(section == 1)
    def _():
        for i in range(batches):
            hand_down(i)

    @pl.when(section < sections - 2)
    def _():
        pass_on(0)
        pass_on(1)

    def project(i, here):
        inv, drop = inv_s[here, :], drop_s[here, :]
        key_flat = kv_s[i, :, 0:kv_width]
        value_flat = kv_s[i, :, kv_width : 2 * kv_width]
        for j in SEND_ORDER:
            cols = slice(j * piece_width, (j + 1) * piece_width)
            projected = nt(key_flat, wk[cols, :]) + nt(value_flat, wv[cols, :])
            for h in range(piece_heads):
                at = head(j * piece_heads + h)
                grad_normed = qb_s[i, :, at] + projected[:, head(h)]
                qb_s[i, :, at] = grad_normed
                low_s[i, :, at] = (
                    up_ref[i, :, at].astype(F32)
                    + inv * gain(j * piece_heads + h) * grad_normed
                    - x_ref[i, :, at].astype(F32) * drop
                ).astype(BF16)

            send_piece(i, j)

    def one_batch(i, carry):
        start = pl.multiple_of(i * tokens, tokens)
        here = pl.ds(start, tokens)
        inv = inv_s[here, :]
        mean = jnp.zeros((tokens, HEAD_DIM), F32)
        for k in KEY_ORDER:

            @pl.when(section < sections - 1)
            def _():
                for j in range(k * PIECES // KV_HEADS, (k + 1) * PIECES // KV_HEADS):
                    slot = piece(up_ref, i, j)
                    remote(slot, slot, us.at[i, j], ur.at[i, j], below).wait_recv()

            upper = jnp.concatenate(
                [up_ref[i, :, head(k * GROUP + h)] for h in range(GROUP)], axis=0
            )
            prob = prob_s[i, k]
            grad_prob = nt(value_s[i, k], upper)
            grad_value = nn(prob.astype(BF16), upper).astype(BF16)
            row_dot = jnp.sum(prob * grad_prob, axis=0, keepdims=True)
            grad_score = (prob * (grad_prob - row_dot) * scale).astype(BF16)
            grad_query = tn(grad_score, key_s[i, k])
            key_back = unrotate(nn(grad_score, query_s[i, k])).astype(BF16)
            kv_s[i, :, head(k)] = key_back
            kv_s[i, :, head(KV_HEADS + k)] = grad_value
            mean = mean + key_back.astype(F32) * pre_k[here, head(k)]
            mean = mean + grad_value.astype(F32) * pre_v[here, head(k)]
            for h in range(GROUP):
                at = head(k * GROUP + h)
                query_back = unrotate(grad_query[h * tokens : (h + 1) * tokens, :])
                qb_s[i, :, at] = query_back
                mean = mean + query_back * (
                    x_ref[i, :, at].astype(F32) * inv * gain(k * GROUP + h)
                )
        @pl.when(section == 0)
        def _():
            for n in range(2):
                kv_copy(i, n).start()

        drop_s[here, :] = inv * inv * (jnp.sum(mean, axis=-1, keepdims=True) * (1.0 / width))

        @pl.when((section > 0) | (i == 0))
        def _():
            project(i, here)

        @pl.when((i == 0) & (section == sections - 1))
        def _():
            attend(1)


        return carry

    lax.fori_loop(0, batches, one_batch, 0)

    @pl.when(section > 0)
    def _():
        for i in range(batches):
            for n in range(2):
                kv_copy(i, n).start()

    @pl.when(section >= sections - 2)
    def _():
        for n in range(3):
            row_copy(n).start()

    @pl.when((xl == 1) & (section > 1))
    def _():
        for i in range(batches):
            hand_down(i)

    @pl.when(section == sections - 1)
    def _():
        for i in range(batches):
            pass_on(i)

    kv_all[xh, c] = kv_s[...]
    for i in range(batches):
        slot = kv_all.at[1 - xh, c, i]
        remote(slot, slot, ks.at[i, 1], kr.at[i, 1], across).wait_recv()
        push(remote(slot, slot, ks.at[i, 2], kr.at[i, 2], partner))
    for n in range(3):
        slot = rows_all.at[near[n][0], near[n][1]]
        remote(slot, slot, ns.at[n], nr.at[n], row_peers[n]).wait_recv()
    for n, a in ((0, xh), (2, 1 - xh)):
        for i in range(batches):
            slot = kv_all.at[a, 1 - c, i]
            remote(slot, slot, ks.at[i, n], kr.at[i, n], partner).wait_recv()

    def column_sums():
        columns = []
        for h in range(heads):
            at = head(h)
            total = jnp.zeros((8, HEAD_DIM), F32)
            for i in range(batches):
                here = slice(i * tokens, (i + 1) * tokens)
                term = qb_s[i, :, at] * x_ref[i, :, at].astype(F32) * inv_s[here, :]
                total = total + jnp.sum(term.reshape(tokens // 8, 8, HEAD_DIM), axis=0)
            columns.append(jnp.sum(total, axis=0, keepdims=True))
        lines = [
            jnp.concatenate([columns[a * 2 * nz + 2 * zz + b] for zz in range(nz)], axis=1)
            for a in range(2)
            for b in range(2)
        ]
        lines.append(jnp.zeros((12, nz * HEAD_DIM), F32))
        col_s[...] = jnp.concatenate(lines, axis=0).astype(BF16)
        col_all[xh, c] = col_s[...]
        for n, peer in enumerate((partner, across)):
            push(remote(col_s, col_all.at[xh, c], cs.at[n], cr.at[n], peer))

    def columns_on():
        slot = col_all.at[1 - xh, c]
        remote(slot, slot, cs.at[1], cr.at[1], across).wait_recv()
        push(remote(slot, slot, cs.at[2], cr.at[2], partner))

    def columns_out():
        for n, a in ((0, xh), (2, 1 - xh)):
            slot = col_all.at[a, 1 - c]
            remote(slot, slot, cs.at[n], cr.at[n], partner).wait_recv()
        own = lax.broadcasted_iota(jnp.int32, (16, nz * HEAD_DIM), 0) == xh * 2 + c
        totals = jnp.zeros((16, nz * HEAD_DIM), F32)
        for a in range(2):
            for b in range(2):
                totals = totals + col_all[a, b].astype(F32)
        line = jnp.sum(jnp.where(own, totals, 0.0), axis=0, keepdims=True)
        for zz in range(nz):
            gsend[zz] = jnp.broadcast_to(line[:, head(zz)], (8, HEAD_DIM))
        for s in range(1, nz):
            push(
                remote(
                    gsend.at[lax.rem(z + s, nz)], grecv.at[s - 1], gs.at[s - 1], gr.at[s - 1],
                    ring[s - 1],
                )
            )

    def write_low():
        for n in range(batches):
            first = plan_ref[0, n] == 0
            for h in range(heads):
                low_out[n, :, head(h)] = jnp.where(
                    first, low_s[0, :, head(h)].astype(F32), low_s[1, :, head(h)].astype(F32)
                ).astype(BF16)

    total_rows = 4 * batches * tokens

    def partial(target, p):
        at = pl.ds(pl.multiple_of(target * HEAD_DIM, HEAD_DIM), HEAD_DIM)
        left = rows_all[:, :, :, at].reshape(total_rows, HEAD_DIM)
        right = kv_all[:, :, :, :, p * kv_width : (p + 1) * kv_width].reshape(total_rows, kv_width)
        return tn(left, right)

    depth = HEAD_DIM // SUBS

    def sum_copy(d, p, t, s):
        return remote(
            sbuf.at[d, p, t, s], rbuf.at[d, p, t, s], rs.at[d, p, t, s], rr.at[d, p, t, s], toward[d]
        )

    for t in range(long_way):
        for p in range(2):
            for d in range(2):
                if t >= hops[p][d]:
                    continue
                steps = hops[p][d] - t
                target = lax.rem(z + (steps if d == 0 else nz - steps), nz)
                mine = partial(target, p)
                for s in range(SUBS):
                    block = mine[s * depth : (s + 1) * depth, :]
                    if t > 0:
                        sum_copy(d, p, t - 1, s).wait_recv()
                        block = block + rbuf[d, p, t - 1, s].astype(F32)
                    sbuf[d, p, t, s] = block.astype(BF16)
                    push(sum_copy(d, p, t, s))
        if t == 0:

            @pl.when(section == 0)
            def _():
                project(batches - 1, slice((batches - 1) * tokens, batches * tokens))

            column_sums()
        elif t == 1:
            columns_on()
            write_low()
        elif t == 2:
            columns_out()
    outs = (key_out, value_out)
    for p in range(2):
        mine = partial(z, p)
        for s in range(SUBS):
            block = mine[s * depth : (s + 1) * depth, :]
            for d in range(2):
                last = hops[p][d] - 1
                sum_copy(d, p, last, s).wait_recv()
                block = block + rbuf[d, p, last, s].astype(F32)
            outs[p][s * depth : (s + 1) * depth, :] = block
    column = gsend[z]
    for s in range(1, nz):
        remote(gsend.at[0], grecv.at[s - 1], gs.at[s - 1], gr.at[s - 1], ring[s - 1]).wait_recv()
        column = column + grecv[s - 1]
    gain_out[...] = column[0:1, :]

    for copy in sends:
        copy.wait_send()
    for n in range(3):
        row_copy(n).wait_send()
    for i in range(batches):
        for n in range(2):
            kv_copy(i, n).wait_send()

    @pl.when(section > 0)
    def _():
        for i in range(batches):
            for j in range(PIECES):
                direct(i, j).wait_send()

    @pl.when(section != sections - 2)
    def _():
        for i in range(batches):
            for n, j in enumerate(DOWN):
                on_parity(j in EVEN_DOWN, j in ODD_DOWN, lambda: onward(i, n).wait_send())

    @pl.when(xl == 1)
    def _():
        for i in range(batches):
            for n in range(len(ODD_UP)):
                over(i, n).wait_send()


def whole(x, cot, wk, wv, gain, plan, ny, nz):
    batches, tokens, width = x.shape
    depth, kv_width = wk.shape
    cosine, sine = rope_tables(tokens, HEAD_DIM)
    rows = batches * tokens
    half = nz // 2
    hop_ring = (2, 2, half, SUBS)
    dma = pltpu.SemaphoreType.DMA
    both = lambda *shape: [dma(shape), dma(shape)]
    via = len(DOWN)
    return pl.pallas_call(
        functools.partial(kernel, ny, nz),
        out_shape=[
            jax.ShapeDtypeStruct((batches, tokens, width), BF16),
            jax.ShapeDtypeStruct((depth, kv_width), F32),
            jax.ShapeDtypeStruct((depth, kv_width), F32),
            jax.ShapeDtypeStruct((1, depth), F32),
        ],
        in_specs=[pl.BlockSpec(memory_space=pltpu.VMEM)] * 5
        + [pl.BlockSpec(memory_space=pltpu.SMEM)]
        + [pl.BlockSpec(memory_space=pltpu.VMEM)] * 2,
        out_specs=[pl.BlockSpec(memory_space=pltpu.VMEM)] * 4,
        scratch_shapes=[
            pltpu.VMEM((2, nz, 2, depth, kv_width), BF16),
            pltpu.VMEM((2, nz, 2, depth, kv_width), BF16),
            pltpu.VMEM((2, 2, nz, 8, depth), F32),
            pltpu.VMEM((8, depth), F32),
            pltpu.VMEM((batches, tokens, width), BF16),
            pltpu.VMEM((batches, tokens, width), BF16),
            pltpu.VMEM((batches, via, tokens, width // PIECES), BF16),
            pltpu.VMEM((batches, len(ODD_UP), tokens, width // PIECES), BF16),
            pltpu.VMEM((rows, width), BF16),
            pltpu.VMEM((2, 2, rows, nz * HEAD_DIM), BF16),
            pltpu.VMEM((2, 2, rows, nz * HEAD_DIM), BF16),
            pltpu.VMEM((batches, KV_HEADS, tokens, HEAD_DIM), BF16),
            pltpu.VMEM((batches, KV_HEADS, tokens, HEAD_DIM), BF16),
            pltpu.VMEM((batches, KV_HEADS, GROUP * tokens, HEAD_DIM), BF16),
            pltpu.VMEM((batches, KV_HEADS, tokens, GROUP * tokens), F32),
            pltpu.VMEM((rows, HEAD_DIM), F32),
            pltpu.VMEM((rows, HEAD_DIM), F32),
            pltpu.VMEM((batches, tokens, width), F32),
            pltpu.VMEM((rows, kv_width), F32),
            pltpu.VMEM((rows, kv_width), F32),
            pltpu.VMEM((batches, tokens, 2 * kv_width), BF16),
            pltpu.VMEM((2, 2, batches, tokens, 2 * kv_width), BF16),
            pltpu.VMEM((16, nz * HEAD_DIM), BF16),
            pltpu.VMEM((2, 2, 16, nz * HEAD_DIM), BF16),
            pltpu.VMEM((*hop_ring, depth // SUBS, kv_width), BF16),
            pltpu.VMEM((*hop_ring, depth // SUBS, kv_width), BF16),
            pltpu.VMEM((nz, 8, HEAD_DIM), F32),
            pltpu.VMEM((nz - 1, 8, HEAD_DIM), F32),
            *both(1),
            *both(2, half, 2, 2),
            *both(1 + 2 * half),
            *both(2, 2, 1 + 2 * half),
            *both(nz - 1),
            *both(3),
            *both(batches, PIECES),
            *both(batches, via),
            dma((batches, via)),
            *both(batches, len(ODD_UP)),
            *both(3),
            *both(batches, 3),
            *both(3),
            *both(*hop_ring),
            *both(nz - 1),
        ],
        compiler_params=pltpu.CompilerParams(
            collective_id=0, has_side_effects=True, vmem_limit_bytes=VMEM_LIMIT
        ),
        name="whole",
    )(x, cot, wk, wv, gain, plan, jnp.asarray(cosine), jnp.asarray(sine))


def solution(mesh):
    sections, dp = mesh.shape["section"], mesh.shape["dp"]
    ny, nz = sections // 2, dp // 4
    split = Mesh(mesh.devices.reshape(ny, 2, 2, nz, 2), ("y", "xl", "xh", "z", "c"))

    def body(inputs, cotangent, norm_gain, key_weight, value_weight, plan):
        low, key_grad, value_grad, gain_grad = whole(
            inputs[0], cotangent, key_weight[0], value_weight[0], norm_gain, plan, ny, nz
        )
        return low[None], key_grad[None], value_grad[None], gain_grad

    placed = (
        P(SECTION, None, DP, None),
        P(None, DP, None),
        P(SECTION, DP),
        P(SECTION, DP, None),
        P(SECTION, DP, None),
        P(SECTION, None),
    )
    return jax.shard_map(
        body,
        mesh=split,
        in_specs=placed,
        out_specs=(
            P(SECTION, None, DP, None),
            P(SECTION, DP, None),
            P(SECTION, DP, None),
            P(SECTION, DP),
        ),
        check_vma=False,
    )
```

```python
import functools
import math

import jax
import jax.numpy as jnp
import numpy as np
from jax import lax
from jax.experimental import pallas as pl
from jax.experimental.pallas import tpu as pltpu
from jax.sharding import Mesh
from jax.sharding import PartitionSpec as P

MESH_ID = pl.DeviceIdType.MESH
KV_HEADS = 4
GROUP = 8
HEAD_DIM = 128
SECTION = ("y", "xl")
DP = ("xh", "z", "c")
eps = 1e-05
rope_base = 500000.0
VMEM_LIMIT = 59 * 1024 * 1024
F32 = jnp.float32
BF16 = jnp.bfloat16

PIECES = 8
EVEN_DOWN = (0, 1, 2)
ODD_DOWN = (0, 2)
ODD_UP = (1,)
DOWN = tuple(sorted(set(EVEN_DOWN + ODD_DOWN)))
SEND_ORDER = (0, 4, 1, 5, 2, 6, 7, 3)
KEY_ORDER = (2, 3, 0, 1)
SUBS = 2


def rope_tables(length, head_dim):
    half = head_dim // 2
    exponent = -(np.arange(half, dtype=np.float32) * np.float32(2.0) / np.float32(head_dim))
    frequency = np.power(np.float32(rope_base), exponent).astype(np.float32)
    angles = np.arange(length, dtype=np.float32)[:, None] * frequency[None, :]
    cosine, sine = np.cos(angles), np.sin(angles)
    return (
        np.concatenate([cosine, cosine], axis=-1).astype(np.float32),
        np.concatenate([-sine, sine], axis=-1).astype(np.float32),
    )


def remote(src, dst, send, recv, peer):
    return pltpu.make_async_remote_copy(
        src_ref=src, dst_ref=dst, send_sem=send, recv_sem=recv, device_id=peer, device_id_type=MESH_ID
    )


def nn(a, b):
    return lax.dot_general(a, b, (((1,), (0,)), ((), ())), preferred_element_type=F32)


def nt(a, b):
    return lax.dot_general(a, b, (((1,), (1,)), ((), ())), preferred_element_type=F32)


def tn(a, b):
    return lax.dot_general(a, b, (((0,), (0,)), ((), ())), preferred_element_type=F32)


def head(h):
    return slice(h * HEAD_DIM, (h + 1) * HEAD_DIM)


def kernel(
    ny, nz,
    x_in, cot_in, wk_in, wv_in, gain_in, plan_ref, cos_in, sin_in,
    low_out, key_out, value_out, gain_out,
    x_ref, wk_ref, wv_ref, gain_ref, cos_ref, sin_ref,
    fk, fv, fg, gown, up_ref, low_s, via_ref, hill_ref, normed_s, out_rows, rows_all, key_s, value_s, query_s,
    prob_s, inv_s, drop_s, qb_s, pre_k, pre_v, kv_s, kv_all, col_s, col_all, sbuf, rbuf, gsend, grecv,
    ld, xs, xr, zs, zr, ws, wr, ds, dr, ls, lr, bs, br,
    us, ur, vs, vr, fs, hs, hr, ns, nr, ks, kr, cs, cr, rs, rr, gs, gr,
):
    y, xl = lax.axis_index("y"), lax.axis_index("xl")
    xh, z, c = lax.axis_index("xh"), lax.axis_index("z"), lax.axis_index("c")
    section, sections = y * 2 + xl, ny * 2
    batches, tokens, width = x_ref.shape
    kv_width = wk_ref.shape[1]
    heads = width // HEAD_DIM
    scale = 1.0 / math.sqrt(HEAD_DIM)

    def section_peer(steps):
        there = lax.rem(section + sections + steps, sections)
        return {"y": there // 2, "xl": lax.rem(there, 2)}

    below, above = section_peer(-1), section_peer(1)
    two_below, two_above = section_peer(-2), section_peer(2)
    three_below, three_above = section_peer(-3), section_peer(3)
    across, partner, corner = {"xh": 1 - xh}, {"c": 1 - c}, {"xh": 1 - xh, "c": 1 - c}
    ring = [{"z": lax.rem(z + s, nz)} for s in range(1, nz)]
    toward = (ring[0], ring[nz - 2])
    long_way, short_way = nz // 2, nz - 1 - nz // 2

    held = (
        (gain_in, gain_ref), (wk_in, wk_ref), (wv_in, wv_ref),
        (x_in, x_ref), (cos_in, cos_ref), (sin_in, sin_ref),
    )
    loads = [pltpu.make_async_copy(src, dst, ld.at[n]) for n, (src, dst) in enumerate(held)]
    for load in loads:
        load.start()
    cot_load = pltpu.make_async_copy(cot_in, up_ref, ld.at[len(held)])

    @pl.when(section == sections - 1)
    def _():
        cot_load.start()

    barrier = pltpu.get_barrier_semaphore()
    greeted = [across, partner, corner, below, above, two_below, two_above]
    greeted += [three_below, three_above] + ring
    for peer in greeted:
        pl.semaphore_signal(barrier, inc=1, device_id=peer, device_id_type=MESH_ID)
    loads[0].wait()
    gown[...] = jnp.broadcast_to(gain_ref[...].astype(F32), gown.shape)
    loads[1].wait()
    loads[2].wait()
    pl.semaphore_wait(barrier, len(greeted))

    sends = []

    def push(copy):
        copy.start()
        sends.append(copy)

    def rotate(v):
        return v * cos_ref[...] + pltpu.roll(v, HEAD_DIM // 2, axis=1) * sin_ref[...]

    def unrotate(v):
        return v * cos_ref[...] - pltpu.roll(v, HEAD_DIM // 2, axis=1) * sin_ref[...]

    def gain(h):
        return fg[h // (2 * nz), h % 2, (h // 2) % nz, 0:1, :]

    sources, fulls = (wk_ref, wv_ref), (fk, fv)
    hops = ((long_way, short_way), (short_way, long_way))

    def place(p, src, steps, core=c):
        row = xh if src == 0 else 1 - xh
        return fulls[p].at[row, lax.rem(z + steps + nz, nz), core]

    def index_of(d, t):
        return 0 if t == 0 else 1 + long_way * d + t - 1

    def steps_of(d, t):
        return -t if d == 0 else t

    def share(p, src, data, slot, index):
        push(remote(data, slot, ds.at[p, src, index], dr.at[p, src, index], partner))

    def ring_copy(data, slot, d, t, src, p):
        return remote(data, slot, zs.at[d, t, src, p], zr.at[d, t, src, p], toward[d])

    def first_moves(p):
        slot = place(p, 0, 0)
        for d in range(2):
            push(ring_copy(sources[p], slot, d, 0, 0, p))
        share(p, 0, sources[p], slot, 0)
        fulls[p][xh, z, c] = sources[p][...]

    def gain_block(row, core, n, peer):
        slot = fg.at[row, core]
        return remote(slot, slot, bs.at[n], br.at[n], peer)

    def row_arrival(p):
        slot = place(p, 1, 0)
        remote(slot, slot, xs.at[p], xr.at[p], across).wait_recv()
        for d in range(2):
            push(ring_copy(slot, slot, d, 0, 1, p))
        share(p, 1, slot, slot, 0)

    def ring_arrival(p, src, d, t):
        if t > hops[p][d]:
            return
        slot = place(p, src, steps_of(d, t))
        ring_copy(slot, slot, d, t - 1, src, p).wait_recv()
        if t < hops[p][d]:
            push(ring_copy(slot, slot, d, t, src, p))
        index = index_of(d, t)
        if p == 1:
            push(remote(slot, slot, ws.at[index], wr.at[index], across))
        share(p, src, slot, slot, index)

    def cross_arrival(d, t):
        if t > hops[1][d]:
            return
        index = index_of(d, t)
        slot = place(1, 1, steps_of(d, t))
        remote(slot, slot, ws.at[index], wr.at[index], across).wait_recv()
        share(1, 1, slot, slot, index)

    def shared_arrivals(p):
        for src in range(2):
            for d in range(2):
                for t in range(hops[p][d] + 1):
                    if t == 0 and d == 1:
                        continue
                    index = index_of(d, t)
                    slot = place(p, src, steps_of(d, t), 1 - c)
                    remote(slot, slot, ds.at[p, src, index], dr.at[p, src, index], partner).wait_recv()

    def mean_square(i):
        here = slice(i * tokens, (i + 1) * tokens)
        total = jnp.zeros((tokens, HEAD_DIM), F32)
        for h in range(heads):
            piece = x_ref[i, :, head(h)].astype(F32)
            total = total + piece * piece
        inv = lax.rsqrt(jnp.sum(total, axis=-1, keepdims=True) * (1.0 / width) + eps)
        inv_s[here, :] = jnp.broadcast_to(inv, (tokens, HEAD_DIM))

    def normalise(i, h):
        here = slice(i * tokens, (i + 1) * tokens)
        piece = x_ref[i, :, head(h)].astype(F32)
        normed = (piece * inv_s[here, :] * gain(h)).astype(BF16)
        normed_s[here, head(h)] = normed
        out_rows[h // (2 * nz), h % 2, here, head((h // 2) % nz)] = normed
        rows = slice((h % GROUP) * tokens, (h % GROUP + 1) * tokens)
        query_s[i, h // GROUP, rows, :] = rotate(normed.astype(F32)).astype(BF16)

    for n in range(1, nz):
        push(remote(gown, fg.at[xh, c, z], ls.at[n - 1], lr.at[n - 1], ring[n - 1]))
    first_moves(0)
    first_moves(1)
    fg[xh, c, z] = gown[...]
    push(remote(sources[0], place(0, 0, 0), xs.at[0], xr.at[0], across))
    push(remote(sources[1], place(1, 0, 0), ws.at[0], wr.at[0], across))
    for load in loads[3:]:
        load.wait()
    mean_square(0)
    mean_square(1)

    def own_gains():
        for n in range(1, nz):
            slot = fg.at[xh, c, lax.rem(z + nz - n, nz)]
            remote(slot, slot, ls.at[n - 1], lr.at[n - 1], ring[n - 1]).wait_recv()
        for n, peer in enumerate((partner, across)):
            push(gain_block(xh, c, n, peer))

    waiting = [(i, h) for i in range(batches) for h in range(heads)]
    share_of = -(-len(waiting) // (2 * long_way - 4))

    def some_work():
        for _ in range(min(share_of, len(waiting))):
            normalise(*waiting.pop(0))

    for t in range(1, long_way + 1):
        for d in range(2):
            ring_arrival(0, 0, d, t)
            ring_arrival(1, 0, d, t)
        if t == 1:
            row_arrival(0)
            own_gains()
        elif t == 2:
            gain_block(1 - xh, c, 1, across).wait_recv()
            push(gain_block(1 - xh, c, 2, partner))
        else:
            some_work()
        for d in range(2):
            ring_arrival(0, 1, d, t)
            if t > 1 or d == 0:
                cross_arrival(d, t - 1)
        if t == 2:
            gain_block(xh, 1 - c, 0, partner).wait_recv()
            gain_block(1 - xh, 1 - c, 2, partner).wait_recv()
        elif t > 2:
            some_work()
    while waiting:
        some_work()
    for d in range(2):
        cross_arrival(d, long_way)
    shared_arrivals(0)
    shared_arrivals(1)
    wk, wv = fk.reshape(width, kv_width), fv.reshape(width, kv_width)

    near = ((xh, 1 - c), (1 - xh, c), (1 - xh, 1 - c))
    row_peers = (partner, across, corner)

    def row_copy(n):
        return remote(
            out_rows.at[near[n][0], near[n][1]], rows_all.at[xh, c], ns.at[n], nr.at[n], row_peers[n]
        )

    rows_all[xh, c] = out_rows[xh, c]

    @pl.when(section < sections - 2)
    def _():
        for n in range(3):
            row_copy(n).start()

    pre_k[...] = nn(normed_s[...], wk[...])
    pre_v[...] = nn(normed_s[...], wv[...])
    m_at = lax.broadcasted_iota(jnp.int32, (tokens, GROUP * tokens), 0)
    l_at = lax.rem(lax.broadcasted_iota(jnp.int32, (tokens, GROUP * tokens), 1), tokens)
    causal = m_at <= l_at

    def attend(i):
        here = slice(i * tokens, (i + 1) * tokens)
        for k in range(KV_HEADS):
            key_s[i, k] = rotate(pre_k[here, head(k)]).astype(BF16)
            value_s[i, k] = pre_v[here, head(k)].astype(BF16)
            scores = nt(key_s[i, k], query_s[i, k]) * scale
            raised = jnp.where(causal, jnp.exp(scores), 0.0)
            prob_s[i, k] = raised / jnp.sum(raised, axis=0, keepdims=True)

    attend(0)

    @pl.when(section < sections - 1)
    def _():
        attend(1)

    piece_width = width // PIECES
    piece_heads = heads // PIECES

    @pl.when(section == sections - 1)
    def _():
        cot_load.wait()

    def piece(ref, i, j):
        return ref.at[i, :, pl.ds(j * piece_width, piece_width)]

    def direct(i, j):
        return remote(piece(low_s, i, j), piece(up_ref, i, j), us.at[i, j], ur.at[i, j], below)

    def roundabout(i, j):
        n = DOWN.index(j)
        return remote(piece(low_s, i, j), via_ref.at[i, n], us.at[i, j], vr.at[i, n], two_below)

    def uphill(i, j):
        n = ODD_UP.index(j)
        return remote(piece(low_s, i, j), hill_ref.at[i, n], us.at[i, j], hr.at[i, n], two_above)

    def over(i, n):
        j = ODD_UP[n]
        return remote(hill_ref.at[i, n], piece(up_ref, i, j), hs.at[i, n], ur.at[i, j], three_below)

    def hand_down(i):
        for n in range(len(ODD_UP)):
            slot = hill_ref.at[i, n]
            remote(slot, slot, hs.at[i, n], hr.at[i, n], three_below).wait_recv()
            over(i, n).start()

    def on_parity(even, odd, run, base=None):
        if even and odd:
            run() if base is None else pl.when(base)(run)
        elif even:
            pl.when((xl == 0) if base is None else (xl == 0) & base)(run)
        elif odd:
            pl.when((xl == 1) if base is None else (xl == 1) & base)(run)

    def send_piece(i, j):
        on_parity(j in EVEN_DOWN, j in ODD_DOWN, lambda: roundabout(i, j).start(), section > 0)
        on_parity(False, j in ODD_UP, lambda: uphill(i, j).start())
        on_parity(
            j not in EVEN_DOWN, j not in ODD_DOWN + ODD_UP, lambda: direct(i, j).start(), section > 0
        )

    def onward(i, n):
        return remote(
            via_ref.at[i, n], piece(up_ref, i, DOWN[n]), fs.at[i, n], ur.at[i, DOWN[n]], above
        )

    def pass_piece(i, n):
        remote(via_ref.at[i, n], via_ref.at[i, n], fs.at[i, n], vr.at[i, n], above).wait_recv()
        onward(i, n).start()

    def pass_on(i):
        for n, j in enumerate(DOWN):
            on_parity(j in EVEN_DOWN, j in ODD_DOWN, functools.partial(pass_piece, i, n))

    def kv_copy(i, n):
        peer = (partner, across)[n]
        return remote(kv_s.at[i], kv_all.at[xh, c, i], ks.at[i, n], kr.at[i, n], peer)

    @pl.when(section == 1)
    def _():
        for i in range(batches):
            hand_down(i)

    @pl.when(section < sections - 2)
    def _():
        pass_on(0)
        pass_on(1)

    def project(i, here):
        inv, drop = inv_s[here, :], drop_s[here, :]
        key_flat = kv_s[i, :, 0:kv_width]
        value_flat = kv_s[i, :, kv_width : 2 * kv_width]
        for j in SEND_ORDER:
            cols = slice(j * piece_width, (j + 1) * piece_width)
            projected = nt(key_flat, wk[cols, :]) + nt(value_flat, wv[cols, :])
            for h in range(piece_heads):
                at = head(j * piece_heads + h)
                grad_normed = qb_s[i, :, at] + projected[:, head(h)]
                qb_s[i, :, at] = grad_normed
                low_s[i, :, at] = (
                    up_ref[i, :, at].astype(F32)
                    + inv * gain(j * piece_heads + h) * grad_normed
                    - x_ref[i, :, at].astype(F32) * drop
                ).astype(BF16)

            send_piece(i, j)

    def one_batch(i, carry):
        start = pl.multiple_of(i * tokens, tokens)
        here = pl.ds(start, tokens)
        inv = inv_s[here, :]
        mean = jnp.zeros((tokens, HEAD_DIM), F32)
        for k in KEY_ORDER:

            @pl.when(section < sections - 1)
            def _():
                for j in range(k * PIECES // KV_HEADS, (k + 1) * PIECES // KV_HEADS):
                    slot = piece(up_ref, i, j)
                    remote(slot, slot, us.at[i, j], ur.at[i, j], below).wait_recv()

            upper = jnp.concatenate(
                [up_ref[i, :, head(k * GROUP + h)] for h in range(GROUP)], axis=0
            )
            prob = prob_s[i, k]
            grad_prob = nt(value_s[i, k], upper)
            grad_value = nn(prob.astype(BF16), upper).astype(BF16)
            row_dot = jnp.sum(prob * grad_prob, axis=0, keepdims=True)
            grad_score = (prob * (grad_prob - row_dot) * scale).astype(BF16)
            grad_query = tn(grad_score, key_s[i, k])
            key_back = unrotate(nn(grad_score, query_s[i, k])).astype(BF16)
            kv_s[i, :, head(k)] = key_back
            kv_s[i, :, head(KV_HEADS + k)] = grad_value
            mean = mean + key_back.astype(F32) * pre_k[here, head(k)]
            mean = mean + grad_value.astype(F32) * pre_v[here, head(k)]
            for h in range(GROUP):
                at = head(k * GROUP + h)
                query_back = unrotate(grad_query[h * tokens : (h + 1) * tokens, :])
                qb_s[i, :, at] = query_back
                mean = mean + query_back * (
                    x_ref[i, :, at].astype(F32) * inv * gain(k * GROUP + h)
                )
        @pl.when(section == 0)
        def _():
            for n in range(2):
                kv_copy(i, n).start()

        drop_s[here, :] = inv * inv * (jnp.sum(mean, axis=-1, keepdims=True) * (1.0 / width))

        @pl.when((section > 0) | (i == 0))
        def _():
            project(i, here)

        @pl.when((i == 0) & (section == sections - 1))
        def _():
            attend(1)


        return carry

    lax.fori_loop(0, batches, one_batch, 0)

    @pl.when(section > 0)
    def _():
        for i in range(batches):
            for n in range(2):
                kv_copy(i, n).start()

    @pl.when(section >= sections - 2)
    def _():
        for n in range(3):
            row_copy(n).start()

    @pl.when((xl == 1) & (section > 1))
    def _():
        for i in range(batches):
            hand_down(i)

    @pl.when(section == sections - 1)
    def _():
        for i in range(batches):
            pass_on(i)

    kv_all[xh, c] = kv_s[...]
    for i in range(batches):
        slot = kv_all.at[1 - xh, c, i]
        remote(slot, slot, ks.at[i, 1], kr.at[i, 1], across).wait_recv()
        push(remote(slot, slot, ks.at[i, 2], kr.at[i, 2], partner))
    for n in range(3):
        slot = rows_all.at[near[n][0], near[n][1]]
        remote(slot, slot, ns.at[n], nr.at[n], row_peers[n]).wait_recv()
    for n, a in ((0, xh), (2, 1 - xh)):
        for i in range(batches):
            slot = kv_all.at[a, 1 - c, i]
            remote(slot, slot, ks.at[i, n], kr.at[i, n], partner).wait_recv()

    def column_sums():
        columns = []
        for h in range(heads):
            at = head(h)
            total = jnp.zeros((8, HEAD_DIM), F32)
            for i in range(batches):
                here = slice(i * tokens, (i + 1) * tokens)
                term = qb_s[i, :, at] * x_ref[i, :, at].astype(F32) * inv_s[here, :]
                total = total + jnp.sum(term.reshape(tokens // 8, 8, HEAD_DIM), axis=0)
            columns.append(jnp.sum(total, axis=0, keepdims=True))
        lines = [
            jnp.concatenate([columns[a * 2 * nz + 2 * zz + b] for zz in range(nz)], axis=1)
            for a in range(2)
            for b in range(2)
        ]
        lines.append(jnp.zeros((12, nz * HEAD_DIM), F32))
        col_s[...] = jnp.concatenate(lines, axis=0).astype(BF16)
        col_all[xh, c] = col_s[...]
        for n, peer in enumerate((partner, across)):
            push(remote(col_s, col_all.at[xh, c], cs.at[n], cr.at[n], peer))

    def columns_on():
        slot = col_all.at[1 - xh, c]
        remote(slot, slot, cs.at[1], cr.at[1], across).wait_recv()
        push(remote(slot, slot, cs.at[2], cr.at[2], partner))

    def columns_out():
        for n, a in ((0, xh), (2, 1 - xh)):
            slot = col_all.at[a, 1 - c]
            remote(slot, slot, cs.at[n], cr.at[n], partner).wait_recv()
        own = lax.broadcasted_iota(jnp.int32, (16, nz * HEAD_DIM), 0) == xh * 2 + c
        totals = jnp.zeros((16, nz * HEAD_DIM), F32)
        for a in range(2):
            for b in range(2):
                totals = totals + col_all[a, b].astype(F32)
        line = jnp.sum(jnp.where(own, totals, 0.0), axis=0, keepdims=True)
        for zz in range(nz):
            gsend[zz] = jnp.broadcast_to(line[:, head(zz)], (8, HEAD_DIM))
        for s in range(1, nz):
            push(
                remote(
                    gsend.at[lax.rem(z + s, nz)], grecv.at[s - 1], gs.at[s - 1], gr.at[s - 1],
                    ring[s - 1],
                )
            )

    def write_low():
        for n in range(batches):
            first = plan_ref[0, n] == 0
            for h in range(heads):
                low_out[n, :, head(h)] = jnp.where(
                    first, low_s[0, :, head(h)].astype(F32), low_s[1, :, head(h)].astype(F32)
                ).astype(BF16)

    total_rows = 4 * batches * tokens

    def partial(target, p):
        at = pl.ds(pl.multiple_of(target * HEAD_DIM, HEAD_DIM), HEAD_DIM)
        left = rows_all[:, :, :, at].reshape(total_rows, HEAD_DIM)
        right = kv_all[:, :, :, :, p * kv_width : (p + 1) * kv_width].reshape(total_rows, kv_width)
        return tn(left, right)

    depth = HEAD_DIM // SUBS

    def sum_copy(d, p, t, s):
        return remote(
            sbuf.at[d, p, t, s], rbuf.at[d, p, t, s], rs.at[d, p, t, s], rr.at[d, p, t, s], toward[d]
        )

    for t in range(long_way):
        for p in range(2):
            for d in range(2):
                if t >= hops[p][d]:
                    continue
                steps = hops[p][d] - t
                target = lax.rem(z + (steps if d == 0 else nz - steps), nz)
                mine = partial(target, p)
                for s in range(SUBS):
                    block = mine[s * depth : (s + 1) * depth, :]
                    if t > 0:
                        sum_copy(d, p, t - 1, s).wait_recv()
                        block = block + rbuf[d, p, t - 1, s].astype(F32)
                    sbuf[d, p, t, s] = block.astype(BF16)
                    push(sum_copy(d, p, t, s))
        if t == 0:

            @pl.when(section == 0)
            def _():
                project(batches - 1, slice((batches - 1) * tokens, batches * tokens))

            column_sums()
        elif t == 1:
            columns_on()
            write_low()
        elif t == 2:
            columns_out()
    outs = (key_out, value_out)
    for p in range(2):
        mine = partial(z, p)
        for s in range(SUBS):
            block = mine[s * depth : (s + 1) * depth, :]
            for d in range(2):
                last = hops[p][d] - 1
                sum_copy(d, p, last, s).wait_recv()
                block = block + rbuf[d, p, last, s].astype(F32)
            outs[p][s * depth : (s + 1) * depth, :] = block
    column = gsend[z]
    for s in range(1, nz):
        remote(gsend.at[0], grecv.at[s - 1], gs.at[s - 1], gr.at[s - 1], ring[s - 1]).wait_recv()
        column = column + grecv[s - 1]
    gain_out[...] = column[0:1, :]

    for copy in sends:
        copy.wait_send()
    for n in range(3):
        row_copy(n).wait_send()
    for i in range(batches):
        for n in range(2):
            kv_copy(i, n).wait_send()

    @pl.when(section > 0)
    def _():
        for i in range(batches):
            for j in range(PIECES):
                direct(i, j).wait_send()

    @pl.when(section != sections - 2)
    def _():
        for i in range(batches):
            for n, j in enumerate(DOWN):
                on_parity(j in EVEN_DOWN, j in ODD_DOWN, lambda: onward(i, n).wait_send())

    @pl.when(xl == 1)
    def _():
        for i in range(batches):
            for n in range(len(ODD_UP)):
                over(i, n).wait_send()


def whole(x, cot, wk, wv, gain, plan, ny, nz):
    batches, tokens, width = x.shape
    depth, kv_width = wk.shape
    cosine, sine = rope_tables(tokens, HEAD_DIM)
    rows = batches * tokens
    half = nz // 2
    hop_ring = (2, 2, half, SUBS)
    dma = pltpu.SemaphoreType.DMA
    both = lambda *shape: [dma(shape), dma(shape)]
    via = len(DOWN)
    return pl.pallas_call(
        functools.partial(kernel, ny, nz),
        out_shape=[
            jax.ShapeDtypeStruct((batches, tokens, width), BF16),
            jax.ShapeDtypeStruct((depth, kv_width), F32),
            jax.ShapeDtypeStruct((depth, kv_width), F32),
            jax.ShapeDtypeStruct((1, depth), F32),
        ],
        in_specs=[pl.BlockSpec(memory_space=pltpu.HBM)] * 5
        + [pl.BlockSpec(memory_space=pltpu.SMEM)]
        + [pl.BlockSpec(memory_space=pltpu.HBM)] * 2,
        out_specs=[pl.BlockSpec(memory_space=pltpu.VMEM)] * 4,
        scratch_shapes=[
            pltpu.VMEM((batches, tokens, width), BF16),
            pltpu.VMEM((depth, kv_width), BF16),
            pltpu.VMEM((depth, kv_width), BF16),
            pltpu.VMEM((1, depth), BF16),
            pltpu.VMEM((tokens, HEAD_DIM), F32),
            pltpu.VMEM((tokens, HEAD_DIM), F32),
            pltpu.VMEM((2, nz, 2, depth, kv_width), BF16),
            pltpu.VMEM((2, nz, 2, depth, kv_width), BF16),
            pltpu.VMEM((2, 2, nz, 8, depth), F32),
            pltpu.VMEM((8, depth), F32),
            pltpu.VMEM((batches, tokens, width), BF16),
            pltpu.VMEM((batches, tokens, width), BF16),
            pltpu.VMEM((batches, via, tokens, width // PIECES), BF16),
            pltpu.VMEM((batches, len(ODD_UP), tokens, width // PIECES), BF16),
            pltpu.VMEM((rows, width), BF16),
            pltpu.VMEM((2, 2, rows, nz * HEAD_DIM), BF16),
            pltpu.VMEM((2, 2, rows, nz * HEAD_DIM), BF16),
            pltpu.VMEM((batches, KV_HEADS, tokens, HEAD_DIM), BF16),
            pltpu.VMEM((batches, KV_HEADS, tokens, HEAD_DIM), BF16),
            pltpu.VMEM((batches, KV_HEADS, GROUP * tokens, HEAD_DIM), BF16),
            pltpu.VMEM((batches, KV_HEADS, tokens, GROUP * tokens), F32),
            pltpu.VMEM((rows, HEAD_DIM), F32),
            pltpu.VMEM((rows, HEAD_DIM), F32),
            pltpu.VMEM((batches, tokens, width), F32),
            pltpu.VMEM((rows, kv_width), F32),
            pltpu.VMEM((rows, kv_width), F32),
            pltpu.VMEM((batches, tokens, 2 * kv_width), BF16),
            pltpu.VMEM((2, 2, batches, tokens, 2 * kv_width), BF16),
            pltpu.VMEM((16, nz * HEAD_DIM), BF16),
            pltpu.VMEM((2, 2, 16, nz * HEAD_DIM), BF16),
            pltpu.VMEM((*hop_ring, depth // SUBS, kv_width), BF16),
            pltpu.VMEM((*hop_ring, depth // SUBS, kv_width), BF16),
            pltpu.VMEM((nz, 8, HEAD_DIM), F32),
            pltpu.VMEM((nz - 1, 8, HEAD_DIM), F32),
            dma((7,)),
            *both(1),
            *both(2, half, 2, 2),
            *both(1 + 2 * half),
            *both(2, 2, 1 + 2 * half),
            *both(nz - 1),
            *both(3),
            *both(batches, PIECES),
            *both(batches, via),
            dma((batches, via)),
            *both(batches, len(ODD_UP)),
            *both(3),
            *both(batches, 3),
            *both(3),
            *both(*hop_ring),
            *both(nz - 1),
        ],
        compiler_params=pltpu.CompilerParams(
            collective_id=0, has_side_effects=True, vmem_limit_bytes=VMEM_LIMIT
        ),
        name="whole",
    )(x, cot, wk, wv, gain, plan, jnp.asarray(cosine), jnp.asarray(sine))


def solution(mesh):
    sections, dp = mesh.shape["section"], mesh.shape["dp"]
    ny, nz = sections // 2, dp // 4
    split = Mesh(mesh.devices.reshape(ny, 2, 2, nz, 2), ("y", "xl", "xh", "z", "c"))

    def body(inputs, cotangent, norm_gain, key_weight, value_weight, plan):
        low, key_grad, value_grad, gain_grad = whole(
            inputs[0], cotangent, key_weight[0], value_weight[0], norm_gain, plan, ny, nz
        )
        return low[None], key_grad[None], value_grad[None], gain_grad

    placed = (
        P(SECTION, None, DP, None),
        P(None, DP, None),
        P(SECTION, DP),
        P(SECTION, DP, None),
        P(SECTION, DP, None),
        P(SECTION, None),
    )
    return jax.shard_map(
        body,
        mesh=split,
        in_specs=placed,
        out_specs=(
            P(SECTION, None, DP, None),
            P(SECTION, DP, None),
            P(SECTION, DP, None),
            P(SECTION, DP),
        ),
        check_vma=False,
    )
```

```python
import functools
import math

import jax
import jax.numpy as jnp
import numpy as np
from jax import lax
from jax.experimental import pallas as pl
from jax.experimental.pallas import tpu as pltpu
from jax.sharding import Mesh
from jax.sharding import PartitionSpec as P

MESH_ID = pl.DeviceIdType.MESH
KV_HEADS = 4
GROUP = 8
HEAD_DIM = 128
SECTION = ("y", "xl")
DP = ("xh", "z", "c")
eps = 1e-05
rope_base = 500000.0
VMEM_LIMIT = 52 * 1024 * 1024
F32 = jnp.float32
BF16 = jnp.bfloat16

PIECES = 8
EVEN_DOWN = (0, 1, 2)
ODD_DOWN = (0, 2)
ODD_UP = (1,)
DOWN = tuple(sorted(set(EVEN_DOWN + ODD_DOWN)))
SEND_ORDER = (0, 4, 1, 5, 2, 6, 7, 3)
KEY_ORDER = (2, 3, 0, 1)
SUBS = 2


def rope_tables(length, head_dim):
    half = head_dim // 2
    exponent = -(np.arange(half, dtype=np.float32) * np.float32(2.0) / np.float32(head_dim))
    frequency = np.power(np.float32(rope_base), exponent).astype(np.float32)
    angles = np.arange(length, dtype=np.float32)[:, None] * frequency[None, :]
    cosine, sine = np.cos(angles), np.sin(angles)
    return (
        np.concatenate([cosine, cosine], axis=-1).astype(np.float32),
        np.concatenate([-sine, sine], axis=-1).astype(np.float32),
    )


def remote(src, dst, send, recv, peer):
    return pltpu.make_async_remote_copy(
        src_ref=src, dst_ref=dst, send_sem=send, recv_sem=recv, device_id=peer, device_id_type=MESH_ID
    )


def nn(a, b):
    return lax.dot_general(a, b, (((1,), (0,)), ((), ())), preferred_element_type=F32)


def nt(a, b):
    return lax.dot_general(a, b, (((1,), (1,)), ((), ())), preferred_element_type=F32)


def tn(a, b):
    return lax.dot_general(a, b, (((0,), (0,)), ((), ())), preferred_element_type=F32)


def head(h):
    return slice(h * HEAD_DIM, (h + 1) * HEAD_DIM)


def kernel(
    ny, nz,
    x_in, cot_in, wk_in, wv_in, gain_in, plan_ref, tables_in,
    low_out, key_out, value_out, gain_out,
    x_ref, wk_ref, wv_ref, gain_ref, tables_ref,
    fk, fv, fg, gown, up_ref, low_s, via_ref, hill_ref, normed_s, out_rows, rows_all, key_s, value_s, query_s,
    prob_s, inv_s, drop_s, qb_s, pre_k, pre_v, kv_s, kv_all, col_s, col_all, sbuf, rbuf, gsend, grecv,
    ld, xs, xr, zs, zr, ws, wr, ds, dr, ls, lr, bs, br,
    us, ur, vs, vr, fs, hs, hr, ns, nr, ks, kr, cs, cr, rs, rr, gs, gr,
):
    y, xl = lax.axis_index("y"), lax.axis_index("xl")
    xh, z, c = lax.axis_index("xh"), lax.axis_index("z"), lax.axis_index("c")
    section, sections = y * 2 + xl, ny * 2
    batches, tokens, width = x_ref.shape
    kv_width = wk_ref.shape[1]
    heads = width // HEAD_DIM
    scale = 1.0 / math.sqrt(HEAD_DIM)

    def section_peer(steps):
        there = lax.rem(section + sections + steps, sections)
        return {"y": there // 2, "xl": lax.rem(there, 2)}

    below, above = section_peer(-1), section_peer(1)
    two_below, two_above = section_peer(-2), section_peer(2)
    three_below, three_above = section_peer(-3), section_peer(3)
    across, partner, corner = {"xh": 1 - xh}, {"c": 1 - c}, {"xh": 1 - xh, "c": 1 - c}
    ring = [{"z": lax.rem(z + s, nz)} for s in range(1, nz)]
    toward = (ring[0], ring[nz - 2])
    long_way, short_way = nz // 2, nz - 1 - nz // 2

    held = (
        (gain_in, gain_ref), (wk_in, wk_ref), (wv_in, wv_ref),
        (x_in, x_ref), (tables_in, tables_ref),
    )
    loads = [pltpu.make_async_copy(src, dst, ld.at[n]) for n, (src, dst) in enumerate(held)]
    for load in loads:
        load.start()
    cot_load = pltpu.make_async_copy(cot_in, up_ref, ld.at[len(held)])

    @pl.when(section == sections - 1)
    def _():
        cot_load.start()

    barrier = pltpu.get_barrier_semaphore()
    greeted = [across, partner, corner, below, above, two_below, two_above]
    greeted += [three_below, three_above] + ring
    for peer in greeted:
        pl.semaphore_signal(barrier, inc=1, device_id=peer, device_id_type=MESH_ID)
    loads[0].wait()
    gown[...] = jnp.broadcast_to(gain_ref[...].astype(F32), gown.shape)
    loads[1].wait()
    loads[2].wait()
    pl.semaphore_wait(barrier, len(greeted))

    sends = []

    def push(copy):
        copy.start()
        sends.append(copy)

    def rotate(v):
        return v * tables_ref[0] + pltpu.roll(v, HEAD_DIM // 2, axis=1) * tables_ref[1]

    def unrotate(v):
        return v * tables_ref[0] - pltpu.roll(v, HEAD_DIM // 2, axis=1) * tables_ref[1]

    def gain(h):
        return fg[h // (2 * nz), h % 2, (h // 2) % nz, 0:1, :]

    sources, fulls = (wk_ref, wv_ref), (fk, fv)
    hops = ((long_way, short_way), (short_way, long_way))

    def place(p, src, steps, core=c):
        row = xh if src == 0 else 1 - xh
        return fulls[p].at[row, lax.rem(z + steps + nz, nz), core]

    def index_of(d, t):
        return 0 if t == 0 else 1 + long_way * d + t - 1

    def steps_of(d, t):
        return -t if d == 0 else t

    def share(p, src, data, slot, index):
        push(remote(data, slot, ds.at[p, src, index], dr.at[p, src, index], partner))

    def ring_copy(data, slot, d, t, src, p):
        return remote(data, slot, zs.at[d, t, src, p], zr.at[d, t, src, p], toward[d])

    def first_moves(p):
        slot = place(p, 0, 0)
        for d in range(2):
            push(ring_copy(sources[p], slot, d, 0, 0, p))
        share(p, 0, sources[p], slot, 0)
        fulls[p][xh, z, c] = sources[p][...]

    def gain_block(row, core, n, peer):
        slot = fg.at[row, core]
        return remote(slot, slot, bs.at[n], br.at[n], peer)

    def row_arrival(p):
        slot = place(p, 1, 0)
        remote(slot, slot, xs.at[p], xr.at[p], across).wait_recv()
        for d in range(2):
            push(ring_copy(slot, slot, d, 0, 1, p))
        share(p, 1, slot, slot, 0)

    def ring_arrival(p, src, d, t):
        if t > hops[p][d]:
            return
        slot = place(p, src, steps_of(d, t))
        ring_copy(slot, slot, d, t - 1, src, p).wait_recv()
        if t < hops[p][d]:
            push(ring_copy(slot, slot, d, t, src, p))
        index = index_of(d, t)
        if p == 1:
            push(remote(slot, slot, ws.at[index], wr.at[index], across))
        share(p, src, slot, slot, index)

    def cross_arrival(d, t):
        if t > hops[1][d]:
            return
        index = index_of(d, t)
        slot = place(1, 1, steps_of(d, t))
        remote(slot, slot, ws.at[index], wr.at[index], across).wait_recv()
        share(1, 1, slot, slot, index)

    def shared_arrivals(p):
        for src in range(2):
            for d in range(2):
                for t in range(hops[p][d] + 1):
                    if t == 0 and d == 1:
                        continue
                    index = index_of(d, t)
                    slot = place(p, src, steps_of(d, t), 1 - c)
                    remote(slot, slot, ds.at[p, src, index], dr.at[p, src, index], partner).wait_recv()

    def mean_square(i):
        here = slice(i * tokens, (i + 1) * tokens)
        total = jnp.zeros((tokens, HEAD_DIM), F32)
        for h in range(heads):
            piece = x_ref[i, :, head(h)].astype(F32)
            total = total + piece * piece
        inv = lax.rsqrt(jnp.sum(total, axis=-1, keepdims=True) * (1.0 / width) + eps)
        inv_s[here, :] = jnp.broadcast_to(inv, (tokens, HEAD_DIM))

    def normalise(i, h):
        here = slice(i * tokens, (i + 1) * tokens)
        piece = x_ref[i, :, head(h)].astype(F32)
        normed = (piece * inv_s[here, :] * gain(h)).astype(BF16)
        normed_s[here, head(h)] = normed
        out_rows[h // (2 * nz), h % 2, here, head((h // 2) % nz)] = normed
        rows = slice((h % GROUP) * tokens, (h % GROUP + 1) * tokens)
        query_s[i, h // GROUP, rows, :] = rotate(normed.astype(F32)).astype(BF16)

    for n in range(1, nz):
        push(remote(gown, fg.at[xh, c, z], ls.at[n - 1], lr.at[n - 1], ring[n - 1]))
    first_moves(0)
    first_moves(1)
    fg[xh, c, z] = gown[...]
    push(remote(sources[0], place(0, 0, 0), xs.at[0], xr.at[0], across))
    push(remote(sources[1], place(1, 0, 0), ws.at[0], wr.at[0], across))
    for load in loads[3:]:
        load.wait()
    mean_square(0)
    mean_square(1)

    def own_gains():
        for n in range(1, nz):
            slot = fg.at[xh, c, lax.rem(z + nz - n, nz)]
            remote(slot, slot, ls.at[n - 1], lr.at[n - 1], ring[n - 1]).wait_recv()
        for n, peer in enumerate((partner, across)):
            push(gain_block(xh, c, n, peer))

    waiting = [(i, h) for i in range(batches) for h in range(heads)]
    share_of = -(-len(waiting) // (2 * long_way - 4))

    def some_work():
        for _ in range(min(share_of, len(waiting))):
            normalise(*waiting.pop(0))

    for t in range(1, long_way + 1):
        for d in range(2):
            ring_arrival(0, 0, d, t)
            ring_arrival(1, 0, d, t)
        if t == 1:
            row_arrival(0)
            own_gains()
        elif t == 2:
            gain_block(1 - xh, c, 1, across).wait_recv()
            push(gain_block(1 - xh, c, 2, partner))
        else:
            some_work()
        for d in range(2):
            ring_arrival(0, 1, d, t)
            if t > 1 or d == 0:
                cross_arrival(d, t - 1)
        if t == 2:
            gain_block(xh, 1 - c, 0, partner).wait_recv()
            gain_block(1 - xh, 1 - c, 2, partner).wait_recv()
        elif t > 2:
            some_work()
    while waiting:
        some_work()
    for d in range(2):
        cross_arrival(d, long_way)
    shared_arrivals(0)
    shared_arrivals(1)
    wk, wv = fk.reshape(width, kv_width), fv.reshape(width, kv_width)

    near = ((xh, 1 - c), (1 - xh, c), (1 - xh, 1 - c))
    row_peers = (partner, across, corner)

    def row_copy(n):
        return remote(
            out_rows.at[near[n][0], near[n][1]], rows_all.at[xh, c], ns.at[n], nr.at[n], row_peers[n]
        )

    rows_all[xh, c] = out_rows[xh, c]

    @pl.when(section < sections - 2)
    def _():
        for n in range(3):
            row_copy(n).start()

    pre_k[...] = nn(normed_s[...], wk[...])
    pre_v[...] = nn(normed_s[...], wv[...])
    m_at = lax.broadcasted_iota(jnp.int32, (tokens, GROUP * tokens), 0)
    l_at = lax.rem(lax.broadcasted_iota(jnp.int32, (tokens, GROUP * tokens), 1), tokens)
    causal = m_at <= l_at

    def attend(i):
        here = slice(i * tokens, (i + 1) * tokens)
        for k in range(KV_HEADS):
            key_s[i, k] = rotate(pre_k[here, head(k)]).astype(BF16)
            value_s[i, k] = pre_v[here, head(k)].astype(BF16)
            scores = nt(key_s[i, k], query_s[i, k]) * scale
            raised = jnp.where(causal, jnp.exp(scores), 0.0)
            prob_s[i, k] = raised / jnp.sum(raised, axis=0, keepdims=True)

    attend(0)

    @pl.when(section < sections - 1)
    def _():
        attend(1)

    piece_width = width // PIECES
    piece_heads = heads // PIECES

    @pl.when(section == sections - 1)
    def _():
        cot_load.wait()

    def piece(ref, i, j):
        return ref.at[i, :, pl.ds(j * piece_width, piece_width)]

    def direct(i, j):
        return remote(piece(low_s, i, j), piece(up_ref, i, j), us.at[i, j], ur.at[i, j], below)

    def roundabout(i, j):
        n = DOWN.index(j)
        return remote(piece(low_s, i, j), via_ref.at[i, n], us.at[i, j], vr.at[i, n], two_below)

    def uphill(i, j):
        n = ODD_UP.index(j)
        return remote(piece(low_s, i, j), hill_ref.at[i, n], us.at[i, j], hr.at[i, n], two_above)

    def over(i, n):
        j = ODD_UP[n]
        return remote(hill_ref.at[i, n], piece(up_ref, i, j), hs.at[i, n], ur.at[i, j], three_below)

    def hand_down(i):
        for n in range(len(ODD_UP)):
            slot = hill_ref.at[i, n]
            remote(slot, slot, hs.at[i, n], hr.at[i, n], three_below).wait_recv()
            over(i, n).start()

    def on_parity(even, odd, run, base=None):
        if even and odd:
            run() if base is None else pl.when(base)(run)
        elif even:
            pl.when((xl == 0) if base is None else (xl == 0) & base)(run)
        elif odd:
            pl.when((xl == 1) if base is None else (xl == 1) & base)(run)

    def send_piece(i, j):
        on_parity(j in EVEN_DOWN, j in ODD_DOWN, lambda: roundabout(i, j).start(), section > 0)
        on_parity(False, j in ODD_UP, lambda: uphill(i, j).start())
        on_parity(
            j not in EVEN_DOWN, j not in ODD_DOWN + ODD_UP, lambda: direct(i, j).start(), section > 0
        )

    def onward(i, n):
        return remote(
            via_ref.at[i, n], piece(up_ref, i, DOWN[n]), fs.at[i, n], ur.at[i, DOWN[n]], above
        )

    def pass_piece(i, n):
        remote(via_ref.at[i, n], via_ref.at[i, n], fs.at[i, n], vr.at[i, n], above).wait_recv()
        onward(i, n).start()

    def pass_on(i):
        for n, j in enumerate(DOWN):
            on_parity(j in EVEN_DOWN, j in ODD_DOWN, functools.partial(pass_piece, i, n))

    def kv_copy(i, n):
        peer = (partner, across)[n]
        return remote(kv_s.at[i], kv_all.at[xh, c, i], ks.at[i, n], kr.at[i, n], peer)

    @pl.when(section == 1)
    def _():
        for i in range(batches):
            hand_down(i)

    @pl.when(section < sections - 2)
    def _():
        pass_on(0)
        pass_on(1)

    def project(i, here):
        inv, drop = inv_s[here, :], drop_s[here, :]
        key_flat = kv_s[i, :, 0:kv_width]
        value_flat = kv_s[i, :, kv_width : 2 * kv_width]
        for j in SEND_ORDER:
            cols = slice(j * piece_width, (j + 1) * piece_width)
            projected = nt(key_flat, wk[cols, :]) + nt(value_flat, wv[cols, :])
            for h in range(piece_heads):
                at = head(j * piece_heads + h)
                grad_normed = qb_s[i, :, at] + projected[:, head(h)]
                qb_s[i, :, at] = grad_normed
                low_s[i, :, at] = (
                    up_ref[i, :, at].astype(F32)
                    + inv * gain(j * piece_heads + h) * grad_normed
                    - x_ref[i, :, at].astype(F32) * drop
                ).astype(BF16)

            send_piece(i, j)

    def one_batch(i, carry):
        start = pl.multiple_of(i * tokens, tokens)
        here = pl.ds(start, tokens)
        inv = inv_s[here, :]
        mean = jnp.zeros((tokens, HEAD_DIM), F32)
        for k in KEY_ORDER:

            @pl.when(section < sections - 1)
            def _():
                for j in range(k * PIECES // KV_HEADS, (k + 1) * PIECES // KV_HEADS):
                    slot = piece(up_ref, i, j)
                    remote(slot, slot, us.at[i, j], ur.at[i, j], below).wait_recv()

            upper = jnp.concatenate(
                [up_ref[i, :, head(k * GROUP + h)] for h in range(GROUP)], axis=0
            )
            prob = prob_s[i, k]
            grad_prob = nt(value_s[i, k], upper)
            grad_value = nn(prob.astype(BF16), upper).astype(BF16)
            row_dot = jnp.sum(prob * grad_prob, axis=0, keepdims=True)
            grad_score = (prob * (grad_prob - row_dot) * scale).astype(BF16)
            grad_query = tn(grad_score, key_s[i, k])
            key_back = unrotate(nn(grad_score, query_s[i, k])).astype(BF16)
            kv_s[i, :, head(k)] = key_back
            kv_s[i, :, head(KV_HEADS + k)] = grad_value
            mean = mean + key_back.astype(F32) * pre_k[here, head(k)]
            mean = mean + grad_value.astype(F32) * pre_v[here, head(k)]
            for h in range(GROUP):
                at = head(k * GROUP + h)
                query_back = unrotate(grad_query[h * tokens : (h + 1) * tokens, :])
                qb_s[i, :, at] = query_back
                mean = mean + query_back * (
                    x_ref[i, :, at].astype(F32) * inv * gain(k * GROUP + h)
                )
        @pl.when(section == 0)
        def _():
            for n in range(2):
                kv_copy(i, n).start()

        drop_s[here, :] = inv * inv * (jnp.sum(mean, axis=-1, keepdims=True) * (1.0 / width))

        @pl.when((section > 0) | (i == 0))
        def _():
            project(i, here)

        @pl.when((i == 0) & (section == sections - 1))
        def _():
            attend(1)


        return carry

    lax.fori_loop(0, batches, one_batch, 0)

    @pl.when(section > 0)
    def _():
        for i in range(batches):
            for n in range(2):
                kv_copy(i, n).start()

    @pl.when(section >= sections - 2)
    def _():
        for n in range(3):
            row_copy(n).start()

    @pl.when((xl == 1) & (section > 1))
    def _():
        for i in range(batches):
            hand_down(i)

    @pl.when(section == sections - 1)
    def _():
        for i in range(batches):
            pass_on(i)

    kv_all[xh, c] = kv_s[...]
    for i in range(batches):
        slot = kv_all.at[1 - xh, c, i]
        remote(slot, slot, ks.at[i, 1], kr.at[i, 1], across).wait_recv()
        push(remote(slot, slot, ks.at[i, 2], kr.at[i, 2], partner))
    for n in range(3):
        slot = rows_all.at[near[n][0], near[n][1]]
        remote(slot, slot, ns.at[n], nr.at[n], row_peers[n]).wait_recv()
    for n, a in ((0, xh), (2, 1 - xh)):
        for i in range(batches):
            slot = kv_all.at[a, 1 - c, i]
            remote(slot, slot, ks.at[i, n], kr.at[i, n], partner).wait_recv()

    def column_sums():
        columns = []
        for h in range(heads):
            at = head(h)
            total = jnp.zeros((8, HEAD_DIM), F32)
            for i in range(batches):
                here = slice(i * tokens, (i + 1) * tokens)
                term = qb_s[i, :, at] * x_ref[i, :, at].astype(F32) * inv_s[here, :]
                total = total + jnp.sum(term.reshape(tokens // 8, 8, HEAD_DIM), axis=0)
            columns.append(jnp.sum(total, axis=0, keepdims=True))
        lines = [
            jnp.concatenate([columns[a * 2 * nz + 2 * zz + b] for zz in range(nz)], axis=1)
            for a in range(2)
            for b in range(2)
        ]
        lines.append(jnp.zeros((12, nz * HEAD_DIM), F32))
        col_s[...] = jnp.concatenate(lines, axis=0).astype(BF16)
        col_all[xh, c] = col_s[...]
        for n, peer in enumerate((partner, across)):
            push(remote(col_s, col_all.at[xh, c], cs.at[n], cr.at[n], peer))

    def columns_on():
        slot = col_all.at[1 - xh, c]
        remote(slot, slot, cs.at[1], cr.at[1], across).wait_recv()
        push(remote(slot, slot, cs.at[2], cr.at[2], partner))

    def columns_out():
        for n, a in ((0, xh), (2, 1 - xh)):
            slot = col_all.at[a, 1 - c]
            remote(slot, slot, cs.at[n], cr.at[n], partner).wait_recv()
        own = lax.broadcasted_iota(jnp.int32, (16, nz * HEAD_DIM), 0) == xh * 2 + c
        totals = jnp.zeros((16, nz * HEAD_DIM), F32)
        for a in range(2):
            for b in range(2):
                totals = totals + col_all[a, b].astype(F32)
        line = jnp.sum(jnp.where(own, totals, 0.0), axis=0, keepdims=True)
        for zz in range(nz):
            gsend[zz] = jnp.broadcast_to(line[:, head(zz)], (8, HEAD_DIM))
        for s in range(1, nz):
            push(
                remote(
                    gsend.at[lax.rem(z + s, nz)], grecv.at[s - 1], gs.at[s - 1], gr.at[s - 1],
                    ring[s - 1],
                )
            )

    def write_low():
        for n in range(batches):
            first = plan_ref[0, n] == 0
            for h in range(heads):
                low_out[n, :, head(h)] = jnp.where(
                    first, low_s[0, :, head(h)].astype(F32), low_s[1, :, head(h)].astype(F32)
                ).astype(BF16)

    total_rows = 4 * batches * tokens

    def partial(target, p):
        at = pl.ds(pl.multiple_of(target * HEAD_DIM, HEAD_DIM), HEAD_DIM)
        left = rows_all[:, :, :, at].reshape(total_rows, HEAD_DIM)
        right = kv_all[:, :, :, :, p * kv_width : (p + 1) * kv_width].reshape(total_rows, kv_width)
        return tn(left, right)

    depth = HEAD_DIM // SUBS

    def sum_copy(d, p, t, s):
        return remote(
            sbuf.at[d, p, t, s], rbuf.at[d, p, t, s], rs.at[d, p, t, s], rr.at[d, p, t, s], toward[d]
        )

    for t in range(long_way):
        for p in range(2):
            for d in range(2):
                if t >= hops[p][d]:
                    continue
                steps = hops[p][d] - t
                target = lax.rem(z + (steps if d == 0 else nz - steps), nz)
                mine = partial(target, p)
                for s in range(SUBS):
                    block = mine[s * depth : (s + 1) * depth, :]
                    if t > 0:
                        sum_copy(d, p, t - 1, s).wait_recv()
                        block = block + rbuf[d, p, t - 1, s].astype(F32)
                    sbuf[d, p, t, s] = block.astype(BF16)
                    push(sum_copy(d, p, t, s))
        if t == 0:

            @pl.when(section == 0)
            def _():
                project(batches - 1, slice((batches - 1) * tokens, batches * tokens))

            column_sums()
        elif t == 1:
            columns_on()
            write_low()
        elif t == 2:
            columns_out()
    outs = (key_out, value_out)
    for p in range(2):
        mine = partial(z, p)
        for s in range(SUBS):
            block = mine[s * depth : (s + 1) * depth, :]
            for d in range(2):
                last = hops[p][d] - 1
                sum_copy(d, p, last, s).wait_recv()
                block = block + rbuf[d, p, last, s].astype(F32)
            outs[p][s * depth : (s + 1) * depth, :] = block
    column = gsend[z]
    for s in range(1, nz):
        remote(gsend.at[0], grecv.at[s - 1], gs.at[s - 1], gr.at[s - 1], ring[s - 1]).wait_recv()
        column = column + grecv[s - 1]
    gain_out[...] = column[0:1, :]

    for copy in sends:
        copy.wait_send()
    for n in range(3):
        row_copy(n).wait_send()
    for i in range(batches):
        for n in range(2):
            kv_copy(i, n).wait_send()

    @pl.when(section > 0)
    def _():
        for i in range(batches):
            for j in range(PIECES):
                direct(i, j).wait_send()

    @pl.when(section != sections - 2)
    def _():
        for i in range(batches):
            for n, j in enumerate(DOWN):
                on_parity(j in EVEN_DOWN, j in ODD_DOWN, lambda: onward(i, n).wait_send())

    @pl.when(xl == 1)
    def _():
        for i in range(batches):
            for n in range(len(ODD_UP)):
                over(i, n).wait_send()


def whole(x, cot, wk, wv, gain, plan, ny, nz):
    batches, tokens, width = x.shape
    depth, kv_width = wk.shape
    cosine, sine = rope_tables(tokens, HEAD_DIM)
    rows = batches * tokens
    half = nz // 2
    hop_ring = (2, 2, half, SUBS)
    dma = pltpu.SemaphoreType.DMA
    both = lambda *shape: [dma(shape), dma(shape)]
    via = len(DOWN)
    return pl.pallas_call(
        functools.partial(kernel, ny, nz),
        out_shape=[
            jax.ShapeDtypeStruct((batches, tokens, width), BF16),
            jax.ShapeDtypeStruct((depth, kv_width), F32),
            jax.ShapeDtypeStruct((depth, kv_width), F32),
            jax.ShapeDtypeStruct((1, depth), F32),
        ],
        in_specs=[pl.BlockSpec(memory_space=pltpu.HBM)] * 5
        + [pl.BlockSpec(memory_space=pltpu.SMEM)]
        + [pl.BlockSpec(memory_space=pltpu.HBM)],
        out_specs=[pl.BlockSpec(memory_space=pltpu.VMEM)] * 4,
        scratch_shapes=[
            pltpu.VMEM((batches, tokens, width), BF16),
            pltpu.VMEM((depth, kv_width), BF16),
            pltpu.VMEM((depth, kv_width), BF16),
            pltpu.VMEM((1, depth), BF16),
            pltpu.VMEM((2, tokens, HEAD_DIM), F32),
            pltpu.VMEM((2, nz, 2, depth, kv_width), BF16),
            pltpu.VMEM((2, nz, 2, depth, kv_width), BF16),
            pltpu.VMEM((2, 2, nz, 8, depth), F32),
            pltpu.VMEM((8, depth), F32),
            pltpu.VMEM((batches, tokens, width), BF16),
            pltpu.VMEM((batches, tokens, width), BF16),
            pltpu.VMEM((batches, via, tokens, width // PIECES), BF16),
            pltpu.VMEM((batches, len(ODD_UP), tokens, width // PIECES), BF16),
            pltpu.VMEM((rows, width), BF16),
            pltpu.VMEM((2, 2, rows, nz * HEAD_DIM), BF16),
            pltpu.VMEM((2, 2, rows, nz * HEAD_DIM), BF16),
            pltpu.VMEM((batches, KV_HEADS, tokens, HEAD_DIM), BF16),
            pltpu.VMEM((batches, KV_HEADS, tokens, HEAD_DIM), BF16),
            pltpu.VMEM((batches, KV_HEADS, GROUP * tokens, HEAD_DIM), BF16),
            pltpu.VMEM((batches, KV_HEADS, tokens, GROUP * tokens), F32),
            pltpu.VMEM((rows, HEAD_DIM), F32),
            pltpu.VMEM((rows, HEAD_DIM), F32),
            pltpu.VMEM((batches, tokens, width), F32),
            pltpu.VMEM((rows, kv_width), F32),
            pltpu.VMEM((rows, kv_width), F32),
            pltpu.VMEM((batches, tokens, 2 * kv_width), BF16),
            pltpu.VMEM((2, 2, batches, tokens, 2 * kv_width), BF16),
            pltpu.VMEM((16, nz * HEAD_DIM), BF16),
            pltpu.VMEM((2, 2, 16, nz * HEAD_DIM), BF16),
            pltpu.VMEM((*hop_ring, depth // SUBS, kv_width), BF16),
            pltpu.VMEM((*hop_ring, depth // SUBS, kv_width), BF16),
            pltpu.VMEM((nz, 8, HEAD_DIM), F32),
            pltpu.VMEM((nz - 1, 8, HEAD_DIM), F32),
            dma((6,)),
            *both(1),
            *both(2, half, 2, 2),
            *both(1 + 2 * half),
            *both(2, 2, 1 + 2 * half),
            *both(nz - 1),
            *both(3),
            *both(batches, PIECES),
            *both(batches, via),
            dma((batches, via)),
            *both(batches, len(ODD_UP)),
            *both(3),
            *both(batches, 3),
            *both(3),
            *both(*hop_ring),
            *both(nz - 1),
        ],
        compiler_params=pltpu.CompilerParams(
            collective_id=0, has_side_effects=True, vmem_limit_bytes=VMEM_LIMIT
        ),
        name="whole",
    )(x, cot, wk, wv, gain, plan, jnp.asarray(np.stack([cosine, sine])))


def solution(mesh):
    sections, dp = mesh.shape["section"], mesh.shape["dp"]
    ny, nz = sections // 2, dp // 4
    split = Mesh(mesh.devices.reshape(ny, 2, 2, nz, 2), ("y", "xl", "xh", "z", "c"))

    def body(inputs, cotangent, norm_gain, key_weight, value_weight, plan):
        low, key_grad, value_grad, gain_grad = whole(
            inputs[0], cotangent, key_weight[0], value_weight[0], norm_gain, plan, ny, nz
        )
        return low[None], key_grad[None], value_grad[None], gain_grad

    placed = (
        P(SECTION, None, DP, None),
        P(None, DP, None),
        P(SECTION, DP),
        P(SECTION, DP, None),
        P(SECTION, DP, None),
        P(SECTION, None),
    )
    return jax.shard_map(
        body,
        mesh=split,
        in_specs=placed,
        out_specs=(
            P(SECTION, None, DP, None),
            P(SECTION, DP, None),
            P(SECTION, DP, None),
            P(SECTION, DP),
        ),
        check_vma=False,
    )
```
